256 devices in a mesh: doc: 4 (over x), mem: 64 (over y, z, core).
Axes of the slice: x: 4, y: 4, z: 8, core: 2. Of those that a mesh axis runs over, the one named last changes fastest.
Arguments:
- queries: bfloat16 [65536, 2048], P(('doc', 'mem')), parts along dimension 0, may hold values from -360 to 360, as said below
- grad_out: bfloat16 [65536, 2048], P(('doc', 'mem')), parts along dimension 0, may hold values from -6 to 6
- mem_keys: bfloat16 [1536, 128, 2048], P(('doc', 'mem')), parts along dimension 0, may hold values from -6 to 6
- mem_values: bfloat16 [1536, 128, 2048], P(('doc', 'mem')), parts along dimension 0, may hold values from -6 to 6
- prev_keys: bfloat16 [512, 128, 2048], P(('doc', 'mem')), parts along dimension 0, may hold values from -6 to 6
- prev_values: bfloat16 [512, 128, 2048], P(('doc', 'mem')), parts along dimension 0, may hold values from -6 to 6
- gate_logit: float32 [16], replicated, may hold values from -2 to 2
- location: int32 [1536], P('doc'), parts along dimension 0, may hold values from 0 to 383, as said below
- top_blocks: int32 [512, 16, 4], P(('doc', 'mem')), parts along dimension 0, may hold values from 0 to 383, as said below
- write_slot: int32 [512], P(('doc', 'mem')), parts along dimension 0, may hold values from 0 to 5, as said below
Outputs:
- attended: bfloat16 [65536, 2048], P(('doc', 'mem')), parts along dimension 0
- query_grad: bfloat16 [65536, 2048], P(('doc', 'mem')), parts along dimension 0
- gate_grad: float32 [64], P('doc'), parts along dimension 0
The draws below stay inside these ranges and needn't reach their ends.
There are 4 independent parts, one for each index of `doc`. The reference program is written for one: setup_inputs(seed, part) draws one part's arguments, and reference() takes and returns one part's arrays. A program takes and returns all parts, laid end to end along the dimension named above; an argument that names none is the same for every part. Nothing has to cross between parts.
Inputs may be any that keep to these rules, and one draw needn't show every extreme that they name: `queries`: values of a row between 6 and 360 in magnitude only through a common row factor. A permutation: memory block j lies in storage slot location[j], which belongs to shard location[j] // 6. `top_blocks`: the 4 blocks of one (b, h) are distinct. Over the rows of one shard, at most 4 entries name blocks whose slots belong to any one shard, and these form at most 2 distinct (block, head) pairs; for each shard both bounds are reached at some shard. `write_slot`: distinct within each aligned group of 2 entries.
All inputs are finite; a program needn't handle non-finite values.
Results may differ from the reference program's by a relative error of at most 0.005.
Values may be sent and summed in bfloat16 or wider, within the bound.
A program may use at most 128 MiB of HBM per device.

```python
import jax
import jax.numpy as jnp
from jax import lax

H = 16
HD = 128
BLK = 128
TOPK = 4
QB_DEV = 2
MB_DEV = 6
NQB = 128
NBLK = 384
TOKENS = 16384
CAP = 2
N_MEM = 64


def routing_tables(key):
    base_key = jax.random.fold_in(key, 7)
    place_key, heat_key, device_key = jax.random.split(base_key, 3)
    location = jax.random.permutation(place_key, NBLK).astype(jnp.int32)
    inverse = jnp.zeros((NBLK,), jnp.int32).at[location].set(jnp.arange(NBLK, dtype=jnp.int32))
    heated = jax.random.randint(heat_key, (N_MEM,), 0, 2)
    half_picks = TOPK // 2
    pool_size = half_picks * (QB_DEV + 1)
    unique_count = H * pool_size
    slot_total = N_MEM * CAP
    slot_owner = jnp.repeat(jnp.arange(N_MEM, dtype=jnp.int32), CAP)

    def one_device(row_key):
        force_key, jitter_key, order_key, shift_key = jax.random.split(row_key, 4)
        forced = jax.random.randint(force_key, (), 0, N_MEM)
        jitter = jax.random.randint(jitter_key, (slot_total,), 0, 65536)
        priority = jnp.where(slot_owner == forced, 0, (heated[slot_owner] + 1) * 65536 + jitter)
        priority = priority * slot_total + jnp.arange(slot_total, dtype=jnp.int32)
        chosen = jnp.argsort(priority)[:unique_count]
        owners_sorted = slot_owner[chosen]
        item_ids = jnp.arange(unique_count, dtype=jnp.int32)
        pool_pos = item_ids % pool_size
        head_ids = item_ids // pool_size
        shared = (pool_pos >= half_picks) & (pool_pos < pool_size - half_picks)
        urgency = jnp.where(shared, 0, 65536) + jax.random.randint(order_key, (unique_count,), 0, 65536)
        urgency = urgency * unique_count + item_ids
        item_order = jnp.argsort(urgency)
        item_owner = jnp.zeros((unique_count,), jnp.int32).at[item_order].set(owners_sorted)
        offsets = jax.random.randint(shift_key, (H,), 0, MB_DEV)
        storage = item_owner * MB_DEV + (pool_pos + offsets[head_ids]) % MB_DEV
        block_pos = jnp.arange(QB_DEV, dtype=jnp.int32)[:, None, None]
        head_pos = jnp.arange(H, dtype=jnp.int32)[None, :, None]
        pick_pos = jnp.arange(TOPK, dtype=jnp.int32)[None, None, :]
        entry_ids = head_pos * pool_size + block_pos * half_picks + pick_pos
        return inverse[storage[entry_ids]]
    device_keys = jax.random.split(device_key, N_MEM)
    chosen_blocks = jax.vmap(one_device)(device_keys).reshape(NQB, H, TOPK)
    return (location, chosen_blocks.astype(jnp.int32))


def draw_location(key, part):
    return routing_tables(key)[0]


def draw_top_blocks(key, part):
    return routing_tables(key)[1]


def draw_write_slot(key, part):
    slot_keys = jax.random.split(jax.random.fold_in(key, 11), N_MEM)

    def pick_slots(row_key):
        return jax.random.permutation(row_key, MB_DEV)[:QB_DEV]
    return jax.vmap(pick_slots)(slot_keys).reshape(NQB).astype(jnp.int32)


def draw_queries(key, part):
    values = jnp.clip(jax.random.normal(jax.random.fold_in(key, 3), (TOKENS, H * HD), jnp.float32), -6.0, 6.0)
    return values.astype(jnp.bfloat16)


def block_levels(stream_key, dims, shards, least, top_value):
    def one(axis_at, blocks):
        steps = jax.random.uniform(jax.random.fold_in(jax.random.fold_in(stream_key, 6), axis_at), (blocks,), jnp.float32, least / len(shards), top_value / len(shards))
        return jnp.repeat(jnp.exp(steps), dims[axis_at] // blocks).reshape((-1,) + (1,) * (len(dims) - axis_at - 1))

    factor_of = one(*shards[0])
    for cut in shards[1:]:
        factor_of = factor_of * one(*cut)
    return factor_of


def bell_draw(own_key, dims, width, limit, pieces=(), kind=jnp.bfloat16):
    loudness = block_levels(own_key, dims, pieces, -0.22, 0.18) if pieces else 1.0
    entries = jax.random.normal(own_key, dims, jnp.float32) * width * loudness
    return jnp.minimum(jnp.maximum(entries, -limit), limit).astype(kind)


def setup_inputs(seed: int = 0, part: int = 0) -> dict:
    splits = jax.random.split(jax.random.key(seed), 11)
    own_keys = jax.random.split(jax.random.fold_in(splits[10], part), 11)
    return {
        "queries": draw_queries(jax.random.fold_in(jax.random.fold_in(splits[10], part), 71), part),
        "grad_out": bell_draw(own_keys[1], (TOKENS, H * HD), 1.0, 6.0, ((0, 64),)),
        "mem_keys": bell_draw(own_keys[2], (NBLK, BLK, H * HD), 1.0, 6.0, ((0, 64),)),
        "mem_values": bell_draw(own_keys[3], (NBLK, BLK, H * HD), 1.0, 6.0, ((0, 64),)),
        "prev_keys": bell_draw(own_keys[4], (NQB, BLK, H * HD), 1.0, 6.0, ((0, 64),)),
        "prev_values": bell_draw(own_keys[5], (NQB, BLK, H * HD), 1.0, 6.0, ((0, 64),)),
        "gate_logit": jnp.clip(jax.random.uniform(splits[6], (H,), jnp.float32, -2.0, 2.0), -2.0, 2.0),
        "location": draw_location(jax.random.fold_in(jax.random.fold_in(splits[10], part), 71), part),
        "top_blocks": draw_top_blocks(jax.random.fold_in(jax.random.fold_in(splits[10], part), 71), part),
        "write_slot": draw_write_slot(jax.random.fold_in(jax.random.fold_in(splits[10], part), 71), part),
    }


def head_major(blocks):
    block_count = blocks.shape[0]
    return blocks.reshape(block_count, BLK, H, HD).transpose(0, 2, 1, 3)


def token_major(blocks):
    return blocks.transpose(0, 2, 1, 3).reshape(TOKENS, H * HD)


def normalized(scores):
    highest = jnp.max(scores, axis=-1, keepdims=True)
    expanded = jnp.exp(scores - highest)
    return expanded / jnp.sum(expanded, axis=-1, keepdims=True)


def rounded(values):
    return lax.optimization_barrier(values.astype(jnp.bfloat16)).astype(jnp.float32)


def attend(query_rows, grad_rows, key_rows, value_rows, share_of, allowed):
    exact = lax.Precision.HIGHEST
    score_scale = HD ** -0.5
    scores = jnp.einsum("hqd,hkd->hqk", query_rows, key_rows, precision=exact) * score_scale
    scores = jnp.where(allowed[None, None, :], scores, -jnp.inf)
    weights = normalized(scores)
    result = jnp.einsum("hqk,hkd->hqd", rounded(weights), value_rows, precision=exact)
    weight_grad = jnp.einsum("hqd,hkd->hqk", grad_rows, value_rows, precision=exact) * share_of[:, None, None]
    score_grad = weights * (weight_grad - jnp.sum(weights * weight_grad, axis=-1, keepdims=True))
    query_grad = jnp.einsum("hqk,hkd->hqd", rounded(score_grad), key_rows, precision=exact)
    return result, query_grad


def reference(queries, grad_out, mem_keys, mem_values, prev_keys, prev_values, gate_logit, location, top_blocks, write_slot):
    target = (jnp.arange(NQB, dtype=jnp.int32) // QB_DEV) * MB_DEV + write_slot.astype(jnp.int32)
    stored_keys = mem_keys.at[target].set(prev_keys).reshape(NBLK, BLK, H, HD)
    stored_values = mem_values.at[target].set(prev_values).reshape(NBLK, BLK, H, HD)
    recent_keys = head_major(prev_keys)
    recent_values = head_major(prev_values)
    older_keys = jnp.concatenate([jnp.zeros_like(recent_keys[:1]), recent_keys[:-1]], axis=0)
    older_values = jnp.concatenate([jnp.zeros_like(recent_values[:1]), recent_values[:-1]], axis=0)
    slot_ids = location[top_blocks].astype(jnp.int32)
    head_ids = jnp.arange(H, dtype=jnp.int32)[:, None]
    mixing = jax.nn.sigmoid(gate_logit.astype(jnp.float32))
    query_heads = head_major(queries.reshape(NQB, BLK, H * HD))
    grad_heads = head_major(grad_out.reshape(NQB, BLK, H * HD))
    block_ids = jnp.arange(NQB, dtype=jnp.int32)

    def one_block(inputs):
        query_rows, grad_rows, slot_row, recent_k, recent_v, older_k, older_v, block_id = inputs
        query_rows = query_rows.astype(jnp.float32)
        grad_rows = grad_rows.astype(jnp.float32)
        memory_keys = stored_keys[slot_row, :, head_ids].reshape(H, TOPK * BLK, HD).astype(jnp.float32)
        memory_values = stored_values[slot_row, :, head_ids].reshape(H, TOPK * BLK, HD).astype(jnp.float32)
        memory_allowed = jnp.ones((TOPK * BLK,), dtype=bool)
        memory_result, memory_grad = attend(query_rows, grad_rows, memory_keys, memory_values, mixing, memory_allowed)
        local_keys = jnp.concatenate([older_k, recent_k], axis=1).astype(jnp.float32)
        local_values = jnp.concatenate([older_v, recent_v], axis=1).astype(jnp.float32)
        local_allowed = jnp.concatenate([jnp.full((BLK,), block_id > 0), jnp.ones((BLK,), dtype=bool)])
        local_result, local_grad = attend(query_rows, grad_rows, local_keys, local_values, 1.0 - mixing, local_allowed)
        blend_of = mixing[:, None, None]
        output = (blend_of * memory_result + (1.0 - blend_of) * local_result).astype(jnp.bfloat16)
        gradient = ((memory_grad + local_grad) * HD ** -0.5).astype(jnp.bfloat16)
        gate_term = jnp.sum(grad_rows * (memory_result - local_result), axis=(1, 2)) * mixing * (1.0 - mixing)
        return output, gradient, gate_term

    outputs, gradients, gate_terms = lax.map(one_block, (query_heads, grad_heads, slot_ids, recent_keys, recent_values, older_keys, older_values, block_ids))
    return token_major(outputs), token_major(gradients), jnp.sum(gate_terms, axis=0)
```

```python
import functools

import jax
import jax.numpy as jnp
from jax import lax
from jax.experimental import pallas as pl
from jax.experimental.pallas import tpu as pltpu
from jax.sharding import PartitionSpec as P

MESH = pl.DeviceIdType.MESH
Z_CHIPS = 8
CORES = 2
LOG2_E = 1.4426950408889634


def route_table(top_blocks, location, stored):
    query_count, head_count, pick_count = top_blocks.shape
    item_count = query_count * head_count * pick_count
    slot_ids = jnp.take(location, top_blocks.reshape(item_count), axis=0)
    owner_ids = slot_ids // stored
    item_ids = jnp.arange(item_count, dtype=jnp.int32)
    head_ids = item_ids // pick_count % head_count
    code_ids = head_ids * stored + slot_ids % stored
    earlier = item_ids[None, :] < item_ids[:, None]
    same_owner = owner_ids[:, None] == owner_ids[None, :]
    pair_ids = slot_ids * head_count + head_ids
    same_pair = pair_ids[:, None] == pair_ids[None, :]
    leading = jnp.logical_not(jnp.any(same_pair & earlier, axis=1))
    lead_rank = jnp.sum(same_owner & earlier & leading[None, :], axis=1)
    position = jnp.sum(jnp.where(same_pair & leading[None, :], lead_rank[None, :], 0), axis=1)
    return (owner_ids, position, code_ids, leading)


def peer_of(step, me, mem_count):
    y_chips = mem_count // (Z_CHIPS * CORES)
    y, z, c = me // (Z_CHIPS * CORES), lax.rem(me // CORES, Z_CHIPS), lax.rem(me, CORES)
    turn = step // Z_CHIPS
    place = lax.rem(step + Z_CHIPS - 1, Z_CHIPS)
    dz = Z_CHIPS // 2 + ((place + 1) // 2) * (1 - 2 * lax.rem(place, 2))
    dy = lax.rem(turn // CORES + 2 * y_chips - dz, y_chips)
    dc = lax.rem(turn, CORES)
    return (lax.rem(y + dy, y_chips) * Z_CHIPS + lax.rem(z + dz, Z_CHIPS)) * CORES + lax.rem(
        c + dc, CORES
    )


def across(a, b):
    return lax.dot_general(a, b, (((1,), (1,)), ((), ())), preferred_element_type=jnp.float32)


def onto(a, b):
    return lax.dot_general(a, b, (((1,), (0,)), ((), ())), preferred_element_type=jnp.float32)


def softmax(raw, scale):
    highest = jnp.max(raw, axis=-1, keepdims=True)
    expanded = jnp.exp2((raw - highest) * (scale * LOG2_E))
    return expanded * (1.0 / jnp.sum(expanded, axis=-1, keepdims=True))


def kernel(
    mem_count,
    head_count,
    pick_count,
    q_hbm,
    g_hbm,
    mk_hbm,
    mv_hbm,
    pk_hbm,
    pv_hbm,
    codes_ref,
    where_ref,
    place_ref,
    gate_ref,
    att_ref,
    qg_ref,
    gate_out_ref,
    q_buf,
    g_buf,
    k_table,
    v_table,
    halo,
    k_send,
    v_send,
    k_got,
    v_got,
    code_got,
    code_smem,
    local_out,
    local_grad,
    weights_buf,
    gate_part,
    gate_send,
    gate_got,
    load_sems,
    send_sems,
    recv_sems,
):
    me = lax.axis_index("mem")
    stored, rows, width = mk_hbm.shape
    query_count = pk_hbm.shape[0]
    dim = width // head_count
    scale = dim**-0.5
    cap = 2
    peers = mem_count - 1

    barrier = pltpu.get_barrier_semaphore()

    def greet(step, _):
        pl.semaphore_signal(
            barrier, inc=1, device_id={"mem": peer_of(step, me, mem_count)}, device_id_type=MESH
        )
        return 0

    lax.fori_loop(1, mem_count, greet, 0)

    table_rows = stored + query_count

    def load_table(source, table, offset, which):
        count = source.shape[0]

        def body(h, _):
            pltpu.make_async_copy(
                source.at[:, :, pl.ds(pl.multiple_of(h * dim, dim), dim)],
                table.at[pl.ds(h * table_rows + offset, count)],
                load_sems.at[which],
            ).start()
            return 0

        lax.fori_loop(0, head_count, body, 0)

    def await_table(source, table, which):
        whole = table.at[pl.ds(0, head_count * source.shape[0])]
        pltpu.make_async_copy(whole, whole, load_sems.at[which]).wait()

    load_table(mk_hbm, k_table, 0, 0)
    load_table(pk_hbm, k_table, stored, 1)
    load_table(mv_hbm, v_table, 0, 2)
    load_table(pv_hbm, v_table, stored, 3)
    loads = [
        pltpu.make_async_copy(q_hbm, q_buf, load_sems.at[4]),
        pltpu.make_async_copy(g_hbm, g_buf, load_sems.at[5]),
    ]
    for load in loads:
        load.start()
    code_got[me] = codes_ref[me]

    pl.semaphore_wait(barrier, peers)

    def remote(src, dst, which, device):
        return pltpu.make_async_remote_copy(
            src_ref=src,
            dst_ref=dst,
            send_sem=send_sems.at[which],
            recv_sem=recv_sems.at[which],
            device_id={"mem": device},
            device_id_type=MESH,
        )

    def send_codes(step, _):
        device = peer_of(step, me, mem_count)
        remote(codes_ref.at[device], code_got.at[me], 0, device).start()
        return 0

    lax.fori_loop(1, mem_count, send_codes, 0)

    following = lax.rem(me + 1, mem_count)
    halo_k = remote(pk_hbm.at[query_count - 1], halo.at[0], 1, following)
    halo_v = remote(pv_hbm.at[query_count - 1], halo.at[1], 2, following)
    halo_k.start()
    halo_v.start()

    some = pl.ds(0, peers)
    remote(codes_ref.at[some], code_got.at[some], 0, following).wait()
    code_copy = pltpu.make_async_copy(code_got, code_smem, load_sems.at[6])
    code_copy.start()
    await_table(mk_hbm, k_table, 0)
    await_table(pk_hbm, k_table, 1)
    await_table(mv_hbm, v_table, 2)
    await_table(pv_hbm, v_table, 3)
    code_copy.wait()

    def gather(table, device, out, at):
        for rank in range(cap):
            out[at + rank] = table[place_ref[code_smem[device, 0, rank]]]

    def serve(table, out, got, which):
        gather(table, peer_of(1, me, mem_count), out, cap)

        def send(step):
            device = peer_of(step, me, mem_count)
            remote(
                out.at[pl.ds(step * cap, cap)], got.at[pl.ds(me * cap, cap)], which, device
            ).start()

        def body(step, _):
            gather(table, peer_of(step, me, mem_count), out, step * cap)
            send(step - 1)
            return 0

        lax.fori_loop(2, mem_count, body, 0)
        gather(table, me, got, me * cap)
        send(peers)

    serve(k_table, k_send, k_got, 3)
    serve(v_table, v_send, v_got, 4)

    for load in loads:
        load.wait()
    halo_k.wait()
    halo_v.wait()

    first = me == 0

    def places(b, h):
        return pl.ds(b * rows, rows), pl.ds(pl.multiple_of(h * dim, dim), dim)

    def mix_of(h):
        return 1.0 / (1.0 + jnp.exp(-jnp.full((1, dim), gate_ref[h], jnp.float32)))

    def local_head(h, _):
        columns = pl.ds(pl.multiple_of(h * dim, dim), dim)
        own = h * table_rows + stored
        rest = 1.0 - mix_of(h)
        part = jnp.zeros((1, dim), jnp.float32)
        for b in range(query_count):
            at = places(b, h)
            q, g = q_buf[at], g_buf[at]
            if b == 0:
                older_k, older_v = halo[0, :, columns], halo[1, :, columns]
            else:
                older_k, older_v = k_table[own + b - 1], v_table[own + b - 1]
            keys = jnp.concatenate([older_k, k_table[own + b]], axis=0)
            values = jnp.concatenate([older_v, v_table[own + b]], axis=0)
            raw = across(q, keys)
            if b == 0:
                column_ids = lax.broadcasted_iota(jnp.int32, raw.shape, 1)
                raw = jnp.where(first & (column_ids < rows), -jnp.inf, raw)
            weights = softmax(raw, scale)
            result = onto(weights.astype(jnp.bfloat16), values)
            weight_grad = across(g, values)
            inner = jnp.sum(weights * weight_grad, axis=-1, keepdims=True)
            score_grad = weights * (weight_grad - inner) * rest[:, :1]
            local_grad[at] = onto(score_grad.astype(jnp.bfloat16), keys)
            local_out[at] = result * rest
            part = part - jnp.sum(g.astype(jnp.float32) * result, axis=0, keepdims=True)
        gate_part[h] = part
        return 0

    lax.fori_loop(0, head_count, local_head, 0)

    def blocks(got, b, h):
        first_item = (b * head_count + h) * pick_count
        return jnp.concatenate([got[where_ref[first_item + k]] for k in range(pick_count)], axis=0)

    everyone = pl.ds(0, peers * cap)
    remote(k_send.at[everyone], k_got.at[everyone], 3, following).wait()

    def memory_weights(h, _):
        for b in range(query_count):
            raw = across(q_buf[places(b, h)], blocks(k_got, b, h))
            weights_buf[b * head_count + h] = softmax(raw, scale)
        return 0

    lax.fori_loop(0, head_count, memory_weights, 0)

    remote(v_send.at[everyone], v_got.at[everyone], 4, following).wait()

    def memory_result(h, _):
        mix = mix_of(h)
        part = gate_part[h]
        for b in range(query_count):
            at = places(b, h)
            weights = weights_buf[b * head_count + h].astype(jnp.bfloat16)
            result = onto(weights, blocks(v_got, b, h))
            att_ref[at] = (mix * result + local_out[at]).astype(jnp.bfloat16)
            part = part + jnp.sum(g_buf[at].astype(jnp.float32) * result, axis=0, keepdims=True)
        gate_part[h] = part
        return 0

    lax.fori_loop(0, head_count, memory_result, 0)

    lane_ids = lax.broadcasted_iota(jnp.int32, (1, dim), 1)
    total = jnp.zeros((1, dim), jnp.float32)
    for h in range(head_count):
        mix = mix_of(h)
        term = jnp.sum(gate_part[h], axis=-1, keepdims=True) * (mix * (1.0 - mix))
        total = jnp.where(lane_ids == h, term, total)
    gate_send[...] = total
    gate_got[me] = total

    def memory_grad(h, _):
        mix = mix_of(h)
        for b in range(query_count):
            at = places(b, h)
            weights = weights_buf[b * head_count + h]
            weight_grad = across(g_buf[at], blocks(v_got, b, h))
            inner = jnp.sum(weights * weight_grad, axis=-1, keepdims=True)
            score_grad = weights * (weight_grad - inner) * mix[:, :1]
            grad = onto(score_grad.astype(jnp.bfloat16), blocks(k_got, b, h))
            qg_ref[at] = ((grad + local_grad[at]) * scale).astype(jnp.bfloat16)
        return 0

    memory_grad(0, 0)

    def send_gate(step, _):
        device = peer_of(step, me, mem_count)
        remote(gate_send, gate_got.at[me], 5, device).start()
        return 0

    lax.fori_loop(1, mem_count, send_gate, 0)
    lax.fori_loop(1, head_count, memory_grad, 0)

    arrived = remote(gate_got.at[some], gate_got.at[some], 5, following)
    arrived.wait()
    gate_out_ref[...] = jnp.sum(gate_got[...], axis=0)


def local(
    queries,
    grad_out,
    mem_keys,
    mem_values,
    prev_keys,
    prev_values,
    gate_logit,
    location,
    top_blocks,
    write_slot,
):
    mem_count = lax.axis_size("mem")
    query_count, head_count, pick_count = top_blocks.shape
    stored, block_rows, row_width = mem_keys.shape
    dim = row_width // head_count
    cap = 2
    owner_ids, position, code_ids, is_live = route_table(top_blocks, location, stored)
    target = jnp.where(is_live, owner_ids * dim + position, mem_count * dim)
    codes = jnp.zeros((mem_count * dim,), jnp.int32).at[target].set(code_ids, mode="drop")
    codes = codes.reshape(mem_count, 1, dim)
    where = owner_ids * cap + position
    place = jnp.arange(stored, dtype=jnp.int32)
    for i in range(query_count):
        place = jnp.where(jnp.arange(stored) == write_slot[i], stored + i, place)
    table_rows = stored + query_count
    place = (jnp.arange(head_count, dtype=jnp.int32)[:, None] * table_rows + place).reshape(-1)
    any_space = pl.BlockSpec(memory_space=pl.ANY)
    smem = pl.BlockSpec(memory_space=pltpu.SMEM)
    vmem = pl.BlockSpec(memory_space=pltpu.VMEM)
    items = mem_count * cap
    attended, query_grad, gate = pl.pallas_call(
        functools.partial(kernel, mem_count, head_count, pick_count),
        out_shape=(
            jax.ShapeDtypeStruct(queries.shape, jnp.bfloat16),
            jax.ShapeDtypeStruct(queries.shape, jnp.bfloat16),
            jax.ShapeDtypeStruct((1, dim), jnp.float32),
        ),
        in_specs=[any_space] * 6 + [vmem, smem, smem, smem],
        out_specs=(vmem, vmem, vmem),
        scratch_shapes=[
            pltpu.VMEM(queries.shape, jnp.bfloat16),
            pltpu.VMEM(queries.shape, jnp.bfloat16),
            pltpu.VMEM((head_count * table_rows, block_rows, dim), jnp.bfloat16),
            pltpu.VMEM((head_count * table_rows, block_rows, dim), jnp.bfloat16),
            pltpu.VMEM((2, block_rows, row_width), jnp.bfloat16),
            pltpu.VMEM((items, block_rows, dim), jnp.bfloat16),
            pltpu.VMEM((items, block_rows, dim), jnp.bfloat16),
            pltpu.VMEM((items, block_rows, dim), jnp.bfloat16),
            pltpu.VMEM((items, block_rows, dim), jnp.bfloat16),
            pltpu.VMEM((mem_count, 1, dim), jnp.int32),
            pltpu.SMEM((mem_count, 1, dim), jnp.int32),
            pltpu.VMEM(queries.shape, jnp.float32),
            pltpu.VMEM(queries.shape, jnp.float32),
            pltpu.VMEM(
                (query_count * head_count, block_rows, pick_count * block_rows), jnp.float32
            ),
            pltpu.VMEM((head_count, 1, dim), jnp.float32),
            pltpu.VMEM((1, dim), jnp.float32),
            pltpu.VMEM((mem_count, 1, dim), jnp.float32),
            pltpu.SemaphoreType.DMA((7,)),
            pltpu.SemaphoreType.DMA((6,)),
            pltpu.SemaphoreType.DMA((6,)),
        ],
        compiler_params=pltpu.CompilerParams(
            collective_id=0, has_side_effects=True, vmem_limit_bytes=60 * 2**20
        ),
        name="retrieve_attend",
    )(
        queries,
        grad_out,
        mem_keys,
        mem_values,
        prev_keys,
        prev_values,
        codes,
        where,
        place,
        gate_logit,
    )
    return (attended, query_grad, gate[0, :head_count])


def solution(mesh):
    in_specs = (
        P(("doc", "mem"), None),
        P(("doc", "mem"), None),
        P(("doc", "mem"), None, None),
        P(("doc", "mem"), None, None),
        P(("doc", "mem"), None, None),
        P(("doc", "mem"), None, None),
        P(),
        P("doc"),
        P(("doc", "mem"), None, None),
        P(("doc", "mem")),
    )
    out_specs = (P(("doc", "mem"), None), P(("doc", "mem"), None), P("doc"))
    return jax.shard_map(local, mesh=mesh, in_specs=in_specs, out_specs=out_specs, check_vma=False)
```

```python
import functools

import jax
import jax.numpy as jnp
from jax import lax
from jax.experimental import pallas as pl
from jax.experimental.pallas import tpu as pltpu
from jax.sharding import PartitionSpec as P

MESH = pl.DeviceIdType.MESH
Z_CHIPS = 8
CORES = 2
LOG2_E = 1.4426950408889634


def route(top_ref, location_ref, write_ref, mem_count, head_count, stored, cap):
    query_count, _, pick_count = top_ref.shape
    items = query_count * head_count * pick_count
    lane = lax.broadcasted_iota(jnp.int32, (1, items), 1)

    def slots_of(h, slots):
        for b in range(query_count):
            for k in range(pick_count):
                item = (b * head_count + h) * pick_count + k
                slots = jnp.where(lane == item, location_ref[top_ref[b, h, k]], slots)
        return slots

    slots = lax.fori_loop(0, head_count, slots_of, jnp.zeros((1, items), jnp.int32))

    def split(value):
        quotient = lax.shift_right_logical(value * ((1 << 18) // stored + 1), 18)
        return quotient, value - quotient * stored

    owners, inside = split(slots)
    heads = lax.shift_right_logical(lane, pick_count.bit_length() - 1) & (head_count - 1)
    codes = heads * stored + inside
    pairs = slots * head_count + heads
    square = (items, items)
    pair_row = jnp.broadcast_to(pairs, square)
    owner_row = jnp.broadcast_to(owners, square)
    same_pair = pair_row == pair_row.T
    same_owner = owner_row == owner_row.T
    row = lax.broadcasted_iota(jnp.int32, square, 0)
    column = lax.broadcasted_iota(jnp.int32, square, 1)

    def count(condition, axis):
        return jnp.sum(jnp.where(condition, 1, 0), axis=axis, keepdims=True)

    lead_of_row = count(same_pair & (column < row), 1) == 0
    lead_of_column = count(same_pair & (row < column), 0) == 0
    rank_of_row = count(same_owner & (column < row) & lead_of_column, 1)
    position = jnp.sum(
        jnp.where(same_pair & lead_of_row, rank_of_row, 0), axis=0, keepdims=True
    )
    asked_shape = (mem_count, items)
    owner = lax.broadcasted_iota(jnp.int32, asked_shape, 0)
    asked_lane = lax.broadcasted_iota(jnp.int32, asked_shape, 1)
    asked = jnp.zeros(asked_shape, jnp.int32)
    for rank in range(cap):
        match = (owners == owner) & lead_of_column & (position == rank)
        code = jnp.sum(jnp.where(match, codes, 0), axis=1, keepdims=True)
        asked = jnp.where(asked_lane == rank, code, asked)
    head, slot = split(lane)
    place = slot
    for i in range(query_count):
        place = jnp.where(slot == write_ref[i], stored + i, place)
    return asked, owners * cap + position, head * (stored + query_count) + place


def peer_of(step, me, mem_count):
    y_chips = mem_count // (Z_CHIPS * CORES)
    y, z, c = me // (Z_CHIPS * CORES), lax.rem(me // CORES, Z_CHIPS), lax.rem(me, CORES)
    turn = step // Z_CHIPS
    place = lax.rem(step + Z_CHIPS - 1, Z_CHIPS)
    dz = Z_CHIPS // 2 + ((place + 1) // 2) * (1 - 2 * lax.rem(place, 2))
    dy = lax.rem(turn // CORES + 2 * y_chips - dz, y_chips)
    dc = lax.rem(turn, CORES)
    return (lax.rem(y + dy, y_chips) * Z_CHIPS + lax.rem(z + dz, Z_CHIPS)) * CORES + lax.rem(
        c + dc, CORES
    )


def across(a, b):
    return lax.dot_general(a, b, (((1,), (1,)), ((), ())), preferred_element_type=jnp.float32)


def onto(a, b):
    return lax.dot_general(a, b, (((1,), (0,)), ((), ())), preferred_element_type=jnp.float32)


def softmax(raw, scale):
    highest = jnp.max(raw, axis=-1, keepdims=True)
    expanded = jnp.exp2((raw - highest) * (scale * LOG2_E))
    return expanded * (1.0 / jnp.sum(expanded, axis=-1, keepdims=True))


def kernel(
    mem_count,
    head_count,
    pick_count,
    q_hbm,
    g_hbm,
    mk_hbm,
    mv_hbm,
    pk_hbm,
    pv_hbm,
    top_ref,
    location_ref,
    write_ref,
    gate_ref,
    att_ref,
    qg_ref,
    gate_out_ref,
    q_buf,
    g_buf,
    k_table,
    v_table,
    halo,
    k_send,
    v_send,
    k_got,
    v_got,
    codes_ref,
    code_got,
    code_smem,
    spots,
    spots_smem,
    local_out,
    local_grad,
    weights_buf,
    gate_part,
    gate_send,
    gate_got,
    load_sems,
    send_sems,
    recv_sems,
):
    me = lax.axis_index("mem")
    stored, rows, width = mk_hbm.shape
    query_count = pk_hbm.shape[0]
    dim = width // head_count
    scale = dim**-0.5
    cap = 2
    peers = mem_count - 1

    barrier = pltpu.get_barrier_semaphore()

    def greet(step, _):
        pl.semaphore_signal(
            barrier, inc=1, device_id={"mem": peer_of(step, me, mem_count)}, device_id_type=MESH
        )
        return 0

    lax.fori_loop(1, mem_count, greet, 0)

    table_rows = stored + query_count

    def load_table(source, table, offset, which):
        count = source.shape[0]

        def body(h, _):
            pltpu.make_async_copy(
                source.at[:, :, pl.ds(pl.multiple_of(h * dim, dim), dim)],
                table.at[pl.ds(h * table_rows + offset, count)],
                load_sems.at[which],
            ).start()
            return 0

        lax.fori_loop(0, head_count, body, 0)

    def await_table(source, table, which):
        whole = table.at[pl.ds(0, head_count * source.shape[0])]
        pltpu.make_async_copy(whole, whole, load_sems.at[which]).wait()

    load_table(mk_hbm, k_table, 0, 0)
    load_table(pk_hbm, k_table, stored, 1)
    load_table(mv_hbm, v_table, 0, 2)
    load_table(pv_hbm, v_table, stored, 3)
    loads = [
        pltpu.make_async_copy(q_hbm, q_buf, load_sems.at[4]),
        pltpu.make_async_copy(g_hbm, g_buf, load_sems.at[5]),
    ]
    for load in loads:
        load.start()
    asked, where, place = route(
        top_ref, location_ref, write_ref, mem_count, head_count, stored, cap
    )
    for device in range(mem_count):
        codes_ref[device] = asked[device : device + 1, :]
    spots[0] = where
    spots[1] = place
    code_got[me] = codes_ref[me]

    pl.semaphore_wait(barrier, peers)

    def remote(src, dst, which, device):
        return pltpu.make_async_remote_copy(
            src_ref=src,
            dst_ref=dst,
            send_sem=send_sems.at[which],
            recv_sem=recv_sems.at[which],
            device_id={"mem": device},
            device_id_type=MESH,
        )

    def send_codes(step, _):
        device = peer_of(step, me, mem_count)
        remote(codes_ref.at[device], code_got.at[me], 0, device).start()
        return 0

    lax.fori_loop(1, mem_count, send_codes, 0)
    spots_copy = pltpu.make_async_copy(spots, spots_smem, load_sems.at[7])
    spots_copy.start()

    following = lax.rem(me + 1, mem_count)
    halo_k = remote(pk_hbm.at[query_count - 1], halo.at[0], 1, following)
    halo_v = remote(pv_hbm.at[query_count - 1], halo.at[1], 2, following)
    halo_k.start()
    halo_v.start()

    some = pl.ds(0, peers)
    remote(codes_ref.at[some], code_got.at[some], 0, following).wait()
    code_copy = pltpu.make_async_copy(code_got, code_smem, load_sems.at[6])
    code_copy.start()
    await_table(mk_hbm, k_table, 0)
    await_table(pk_hbm, k_table, 1)
    await_table(mv_hbm, v_table, 2)
    await_table(pv_hbm, v_table, 3)
    code_copy.wait()
    spots_copy.wait()

    def gather(table, device, out, at):
        for rank in range(cap):
            out[at + rank] = table[spots_smem[1, 0, code_smem[device, 0, rank]]]

    def serve(table, out, got, which):
        gather(table, peer_of(1, me, mem_count), out, cap)

        def send(step):
            device = peer_of(step, me, mem_count)
            remote(
                out.at[pl.ds(step * cap, cap)], got.at[pl.ds(me * cap, cap)], which, device
            ).start()

        def body(step, _):
            gather(table, peer_of(step, me, mem_count), out, step * cap)
            send(step - 1)
            return 0

        lax.fori_loop(2, mem_count, body, 0)
        gather(table, me, got, me * cap)
        send(peers)

    serve(k_table, k_send, k_got, 3)
    serve(v_table, v_send, v_got, 4)

    for load in loads:
        load.wait()
    halo_k.wait()
    halo_v.wait()

    first = me == 0

    def places(b, h):
        return pl.ds(b * rows, rows), pl.ds(pl.multiple_of(h * dim, dim), dim)

    def mix_of(h):
        return 1.0 / (1.0 + jnp.exp(-jnp.full((1, dim), gate_ref[h], jnp.float32)))

    def local_head(h, _):
        columns = pl.ds(pl.multiple_of(h * dim, dim), dim)
        own = h * table_rows + stored
        rest = 1.0 - mix_of(h)
        part = jnp.zeros((1, dim), jnp.float32)
        for b in range(query_count):
            at = places(b, h)
            q, g = q_buf[at], g_buf[at]
            if b == 0:
                older_k, older_v = halo[0, :, columns], halo[1, :, columns]
            else:
                older_k, older_v = k_table[own + b - 1], v_table[own + b - 1]
            keys = jnp.concatenate([older_k, k_table[own + b]], axis=0)
            values = jnp.concatenate([older_v, v_table[own + b]], axis=0)
            raw = across(q, keys)
            if b == 0:
                column_ids = lax.broadcasted_iota(jnp.int32, raw.shape, 1)
                raw = jnp.where(first & (column_ids < rows), -jnp.inf, raw)
            weights = softmax(raw, scale)
            result = onto(weights.astype(jnp.bfloat16), values)
            weight_grad = across(g, values)
            inner = jnp.sum(weights * weight_grad, axis=-1, keepdims=True)
            score_grad = weights * (weight_grad - inner) * rest[:, :1]
            local_grad[at] = onto(score_grad.astype(jnp.bfloat16), keys)
            local_out[at] = result * rest
            part = part - jnp.sum(g.astype(jnp.float32) * result, axis=0, keepdims=True)
        gate_part[h] = part
        return 0

    lax.fori_loop(0, head_count, local_head, 0)

    def blocks(got, b, h):
        first_item = (b * head_count + h) * pick_count
        return jnp.concatenate([got[spots_smem[0, 0, first_item + k]] for k in range(pick_count)], axis=0)

    everyone = pl.ds(0, peers * cap)
    remote(k_send.at[everyone], k_got.at[everyone], 3, following).wait()

    def memory_weights(h, _):
        for b in range(query_count):
            raw = across(q_buf[places(b, h)], blocks(k_got, b, h))
            weights_buf[b * head_count + h] = softmax(raw, scale)
        return 0

    lax.fori_loop(0, head_count, memory_weights, 0)

    remote(v_send.at[everyone], v_got.at[everyone], 4, following).wait()

    def memory_result(h, _):
        mix = mix_of(h)
        part = gate_part[h]
        for b in range(query_count):
            at = places(b, h)
            weights = weights_buf[b * head_count + h].astype(jnp.bfloat16)
            result = onto(weights, blocks(v_got, b, h))
            att_ref[at] = (mix * result + local_out[at]).astype(jnp.bfloat16)
            part = part + jnp.sum(g_buf[at].astype(jnp.float32) * result, axis=0, keepdims=True)
        gate_part[h] = part
        return 0

    lax.fori_loop(0, head_count, memory_result, 0)

    lane_ids = lax.broadcasted_iota(jnp.int32, (1, dim), 1)
    total = jnp.zeros((1, dim), jnp.float32)
    for h in range(head_count):
        mix = mix_of(h)
        term = jnp.sum(gate_part[h], axis=-1, keepdims=True) * (mix * (1.0 - mix))
        total = jnp.where(lane_ids == h, term, total)
    gate_send[...] = total
    gate_got[me] = total

    def memory_grad(h, _):
        mix = mix_of(h)
        for b in range(query_count):
            at = places(b, h)
            weights = weights_buf[b * head_count + h]
            weight_grad = across(g_buf[at], blocks(v_got, b, h))
            inner = jnp.sum(weights * weight_grad, axis=-1, keepdims=True)
            score_grad = weights * (weight_grad - inner) * mix[:, :1]
            grad = onto(score_grad.astype(jnp.bfloat16), blocks(k_got, b, h))
            qg_ref[at] = ((grad + local_grad[at]) * scale).astype(jnp.bfloat16)
        return 0

    memory_grad(0, 0)

    def send_gate(step, _):
        device = peer_of(step, me, mem_count)
        remote(gate_send, gate_got.at[me], 5, device).start()
        return 0

    lax.fori_loop(1, mem_count, send_gate, 0)
    lax.fori_loop(1, head_count, memory_grad, 0)

    arrived = remote(gate_got.at[some], gate_got.at[some], 5, following)
    arrived.wait()
    gate_out_ref[...] = jnp.sum(gate_got[...], axis=0)


def publish(att_ref, qg_ref, gate_ref, att_hbm, qg_hbm, gate_out, sems):
    copies = [
        pltpu.make_async_copy(att_ref, att_hbm, sems.at[0]),
        pltpu.make_async_copy(qg_ref, qg_hbm, sems.at[1]),
    ]
    for copy in copies:
        copy.start()
    gate_out[...] = gate_ref[0, : gate_out.shape[0]]
    for copy in copies:
        copy.wait()


def local(
    queries,
    grad_out,
    mem_keys,
    mem_values,
    prev_keys,
    prev_values,
    gate_logit,
    location,
    top_blocks,
    write_slot,
):
    mem_count = lax.axis_size("mem")
    query_count, head_count, pick_count = top_blocks.shape
    stored, block_rows, row_width = mem_keys.shape
    dim = row_width // head_count
    cap = 2
    table_rows = stored + query_count
    any_space = pl.BlockSpec(memory_space=pl.ANY)
    smem = pl.BlockSpec(memory_space=pltpu.SMEM)
    vmem = pl.BlockSpec(memory_space=pltpu.VMEM)
    items = mem_count * cap
    attended, query_grad, gate = pl.pallas_call(
        functools.partial(kernel, mem_count, head_count, pick_count),
        out_shape=(
            pltpu.VMEM(queries.shape, jnp.bfloat16),
            pltpu.VMEM(queries.shape, jnp.bfloat16),
            pltpu.VMEM((1, dim), jnp.float32),
        ),
        in_specs=[any_space] * 6 + [smem] * 4,
        out_specs=(vmem, vmem, vmem),
        scratch_shapes=[
            pltpu.VMEM(queries.shape, jnp.bfloat16),
            pltpu.VMEM(queries.shape, jnp.bfloat16),
            pltpu.VMEM((head_count * table_rows, block_rows, dim), jnp.bfloat16),
            pltpu.VMEM((head_count * table_rows, block_rows, dim), jnp.bfloat16),
            pltpu.VMEM((2, block_rows, row_width), jnp.bfloat16),
            pltpu.VMEM((items, block_rows, dim), jnp.bfloat16),
            pltpu.VMEM((items, block_rows, dim), jnp.bfloat16),
            pltpu.VMEM((items, block_rows, dim), jnp.bfloat16),
            pltpu.VMEM((items, block_rows, dim), jnp.bfloat16),
            pltpu.VMEM((mem_count, 1, dim), jnp.int32),
            pltpu.VMEM((mem_count, 1, dim), jnp.int32),
            pltpu.SMEM((mem_count, 1, dim), jnp.int32),
            pltpu.VMEM((2, 1, dim), jnp.int32),
            pltpu.SMEM((2, 1, dim), jnp.int32),
            pltpu.VMEM(queries.shape, jnp.float32),
            pltpu.VMEM(queries.shape, jnp.float32),
            pltpu.VMEM(
                (query_count * head_count, block_rows, pick_count * block_rows), jnp.float32
            ),
            pltpu.VMEM((head_count, 1, dim), jnp.float32),
            pltpu.VMEM((1, dim), jnp.float32),
            pltpu.VMEM((mem_count, 1, dim), jnp.float32),
            pltpu.SemaphoreType.DMA((8,)),
            pltpu.SemaphoreType.DMA((6,)),
            pltpu.SemaphoreType.DMA((6,)),
        ],
        compiler_params=pltpu.CompilerParams(
            collective_id=0, has_side_effects=True, vmem_limit_bytes=60 * 2**20
        ),
        name="retrieve_attend",
    )(
        queries,
        grad_out,
        mem_keys,
        mem_values,
        prev_keys,
        prev_values,
        top_blocks,
        location,
        write_slot,
        gate_logit,
    )
    return pl.pallas_call(
        publish,
        out_shape=(
            jax.ShapeDtypeStruct(queries.shape, jnp.bfloat16),
            jax.ShapeDtypeStruct(queries.shape, jnp.bfloat16),
            jax.ShapeDtypeStruct((head_count,), jnp.float32),
        ),
        in_specs=[vmem] * 3,
        out_specs=(any_space, any_space, vmem),
        scratch_shapes=[pltpu.SemaphoreType.DMA((2,))],
        name="publish",
    )(*(pltpu.with_memory_space_constraint(x, pltpu.VMEM) for x in (attended, query_grad, gate)))


def solution(mesh):
    in_specs = (
        P(("doc", "mem"), None),
        P(("doc", "mem"), None),
        P(("doc", "mem"), None, None),
        P(("doc", "mem"), None, None),
        P(("doc", "mem"), None, None),
        P(("doc", "mem"), None, None),
        P(),
        P("doc"),
        P(("doc", "mem"), None, None),
        P(("doc", "mem")),
    )
    out_specs = (P(("doc", "mem"), None), P(("doc", "mem"), None), P("doc"))
    return jax.shard_map(local, mesh=mesh, in_specs=in_specs, out_specs=out_specs, check_vma=False)
```

```python
import functools

import jax
import jax.numpy as jnp
from jax import lax
from jax.experimental import pallas as pl
from jax.experimental.pallas import tpu as pltpu
from jax.sharding import PartitionSpec as P

MESH = pl.DeviceIdType.MESH
Z_CHIPS = 8
CORES = 2
LOG2_E = 1.4426950408889634


def route(top_ref, location_ref, write_ref, mem_count, head_count, stored, cap):
    query_count, pick_count, _ = top_ref.shape
    items = query_count * head_count * pick_count
    lane = lax.broadcasted_iota(jnp.int32, (1, items), 1)

    def slots_of(h, slots):
        for b in range(query_count):
            for k in range(pick_count):
                item = (b * head_count + h) * pick_count + k
                slots = jnp.where(lane == item, location_ref[top_ref[b, k, h]], slots)
        return slots

    slots = lax.fori_loop(0, head_count, slots_of, jnp.zeros((1, items), jnp.int32))

    def split(value):
        quotient = lax.shift_right_logical(value * ((1 << 18) // stored + 1), 18)
        return quotient, value - quotient * stored

    owners, inside = split(slots)
    heads = lax.shift_right_logical(lane, pick_count.bit_length() - 1) & (head_count - 1)
    codes = heads * stored + inside
    pairs = slots * head_count + heads
    square = (items, items)
    pair_row = jnp.broadcast_to(pairs, square)
    owner_row = jnp.broadcast_to(owners, square)
    same_pair = pair_row == pair_row.T
    same_owner = owner_row == owner_row.T
    row = lax.broadcasted_iota(jnp.int32, square, 0)
    column = lax.broadcasted_iota(jnp.int32, square, 1)

    def count(condition, axis):
        return jnp.sum(jnp.where(condition, 1, 0), axis=axis, keepdims=True)

    lead_of_row = count(same_pair & (column < row), 1) == 0
    lead_of_column = count(same_pair & (row < column), 0) == 0
    rank_of_row = count(same_owner & (column < row) & lead_of_column, 1)
    position = jnp.sum(
        jnp.where(same_pair & lead_of_row, rank_of_row, 0), axis=0, keepdims=True
    )
    asked_shape = (mem_count, items)
    owner = lax.broadcasted_iota(jnp.int32, asked_shape, 0)
    asked_lane = lax.broadcasted_iota(jnp.int32, asked_shape, 1)
    asked = jnp.zeros(asked_shape, jnp.int32)
    for rank in range(cap):
        match = (owners == owner) & lead_of_column & (position == rank)
        code = jnp.sum(jnp.where(match, codes, 0), axis=1, keepdims=True)
        asked = jnp.where(asked_lane == rank, code, asked)
    head, slot = split(lane)
    place = slot
    for i in range(query_count):
        place = jnp.where(slot == write_ref[i], stored + i, place)
    return asked, owners * cap + position, head * (stored + query_count) + place


def peer_of(step, me, mem_count):
    y_chips = mem_count // (Z_CHIPS * CORES)
    y, z, c = me // (Z_CHIPS * CORES), lax.rem(me // CORES, Z_CHIPS), lax.rem(me, CORES)
    turn = step // Z_CHIPS
    place = lax.rem(step + Z_CHIPS - 1, Z_CHIPS)
    dz = Z_CHIPS // 2 + ((place + 1) // 2) * (1 - 2 * lax.rem(place, 2))
    dy = lax.rem(turn // CORES + 2 * y_chips - dz, y_chips)
    dc = lax.rem(turn, CORES)
    return (lax.rem(y + dy, y_chips) * Z_CHIPS + lax.rem(z + dz, Z_CHIPS)) * CORES + lax.rem(
        c + dc, CORES
    )


def across(a, b):
    return lax.dot_general(a, b, (((1,), (1,)), ((), ())), preferred_element_type=jnp.float32)


def onto(a, b):
    return lax.dot_general(a, b, (((1,), (0,)), ((), ())), preferred_element_type=jnp.float32)


def softmax(raw, scale):
    highest = jnp.max(raw, axis=-1, keepdims=True)
    expanded = jnp.exp2((raw - highest) * (scale * LOG2_E))
    return expanded * (1.0 / jnp.sum(expanded, axis=-1, keepdims=True))


def kernel(
    mem_count,
    head_count,
    pick_count,
    q_hbm,
    g_hbm,
    mk_hbm,
    mv_hbm,
    pk_hbm,
    pv_hbm,
    top_ref,
    location_ref,
    write_ref,
    gate_ref,
    att_ref,
    qg_ref,
    gate_out_ref,
    q_buf,
    g_buf,
    k_table,
    v_table,
    halo,
    k_send,
    v_send,
    k_got,
    v_got,
    codes_ref,
    code_got,
    code_smem,
    spots,
    spots_smem,
    local_out,
    local_grad,
    weights_buf,
    mixed_buf,
    gate_part,
    gate_send,
    gate_got,
    load_sems,
    send_sems,
    recv_sems,
):
    me = lax.axis_index("mem")
    stored, rows, width = mk_hbm.shape
    query_count = pk_hbm.shape[0]
    dim = width // head_count
    scale = dim**-0.5
    cap = 2
    peers = mem_count - 1

    barrier = pltpu.get_barrier_semaphore()

    def greet(step, _):
        pl.semaphore_signal(
            barrier, inc=1, device_id={"mem": peer_of(step, me, mem_count)}, device_id_type=MESH
        )
        return 0

    lax.fori_loop(1, mem_count, greet, 0)

    table_rows = stored + query_count

    def load_table(source, table, offset, which):
        count = source.shape[0]

        def body(h, _):
            pltpu.make_async_copy(
                source.at[:, :, pl.ds(pl.multiple_of(h * dim, dim), dim)],
                table.at[pl.ds(h * table_rows + offset, count)],
                load_sems.at[which],
            ).start()
            return 0

        lax.fori_loop(0, head_count, body, 0)

    def await_table(source, table, which):
        whole = table.at[pl.ds(0, head_count * source.shape[0])]
        pltpu.make_async_copy(whole, whole, load_sems.at[which]).wait()

    load_table(mk_hbm, k_table, 0, 0)
    load_table(pk_hbm, k_table, stored, 1)
    load_table(mv_hbm, v_table, 0, 2)
    load_table(pv_hbm, v_table, stored, 3)
    loads = [
        pltpu.make_async_copy(q_hbm, q_buf, load_sems.at[4]),
        pltpu.make_async_copy(g_hbm, g_buf, load_sems.at[5]),
    ]
    for load in loads:
        load.start()
    asked, where, place = route(
        top_ref, location_ref, write_ref, mem_count, head_count, stored, cap
    )
    for device in range(mem_count):
        codes_ref[device] = asked[device : device + 1, :]
    spots[0] = where
    spots[1] = place
    code_got[me] = codes_ref[me]

    pl.semaphore_wait(barrier, peers)

    def remote(src, dst, which, device):
        return pltpu.make_async_remote_copy(
            src_ref=src,
            dst_ref=dst,
            send_sem=send_sems.at[which],
            recv_sem=recv_sems.at[which],
            device_id={"mem": device},
            device_id_type=MESH,
        )

    def send_codes(step, _):
        device = peer_of(step, me, mem_count)
        remote(codes_ref.at[device], code_got.at[me], 0, device).start()
        return 0

    lax.fori_loop(1, mem_count, send_codes, 0)
    spots_copy = pltpu.make_async_copy(spots, spots_smem, load_sems.at[7])
    spots_copy.start()

    following = lax.rem(me + 1, mem_count)
    halo_k = remote(pk_hbm.at[query_count - 1], halo.at[0], 1, following)
    halo_v = remote(pv_hbm.at[query_count - 1], halo.at[1], 2, following)
    halo_k.start()
    halo_v.start()

    some = pl.ds(0, peers)
    remote(codes_ref.at[some], code_got.at[some], 0, following).wait()
    code_copy = pltpu.make_async_copy(code_got, code_smem, load_sems.at[6])
    code_copy.start()
    await_table(mk_hbm, k_table, 0)
    await_table(pk_hbm, k_table, 1)
    await_table(mv_hbm, v_table, 2)
    await_table(pv_hbm, v_table, 3)
    code_copy.wait()
    spots_copy.wait()

    def gather(table, device, out, at):
        for rank in range(cap):
            out[at + rank] = table[spots_smem[1, 0, code_smem[device, 0, rank]]]

    def serve(table, out, got, which):
        gather(table, peer_of(1, me, mem_count), out, cap)

        def send(step):
            device = peer_of(step, me, mem_count)
            remote(
                out.at[pl.ds(step * cap, cap)], got.at[pl.ds(me * cap, cap)], which, device
            ).start()

        def body(step, _):
            gather(table, peer_of(step, me, mem_count), out, step * cap)
            send(step - 1)
            return 0

        lax.fori_loop(2, mem_count, body, 0)
        gather(table, me, got, me * cap)
        send(peers)

    serve(k_table, k_send, k_got, 3)
    serve(v_table, v_send, v_got, 4)

    for load in loads:
        load.wait()
    halo_k.wait()
    halo_v.wait()

    first = me == 0

    def places(b, h):
        return pl.ds(b * rows, rows), pl.ds(pl.multiple_of(h * dim, dim), dim)

    def mix_of(h):
        return 1.0 / (1.0 + jnp.exp(-jnp.full((1, dim), gate_ref[h], jnp.float32)))

    def local_head(h, _):
        columns = pl.ds(pl.multiple_of(h * dim, dim), dim)
        own = h * table_rows + stored
        rest = 1.0 - mix_of(h)
        part = jnp.zeros((1, dim), jnp.float32)
        for b in range(query_count):
            at = places(b, h)
            q, g = q_buf[at], g_buf[at]
            if b == 0:
                older_k, older_v = halo[0, :, columns], halo[1, :, columns]
            else:
                older_k, older_v = k_table[own + b - 1], v_table[own + b - 1]
            keys = jnp.concatenate([older_k, k_table[own + b]], axis=0)
            values = jnp.concatenate([older_v, v_table[own + b]], axis=0)
            raw = across(q, keys)
            if b == 0:
                column_ids = lax.broadcasted_iota(jnp.int32, raw.shape, 1)
                raw = jnp.where(first & (column_ids < rows), -jnp.inf, raw)
            weights = softmax(raw, scale)
            result = onto(weights.astype(jnp.bfloat16), values)
            weight_grad = across(g, values)
            inner = jnp.sum(weights * weight_grad, axis=-1, keepdims=True)
            score_grad = weights * (weight_grad - inner) * rest[:, :1]
            local_grad[at] = onto(score_grad.astype(jnp.bfloat16), keys)
            local_out[at] = result * rest
            part = part - jnp.sum(g.astype(jnp.float32) * result, axis=0, keepdims=True)
        gate_part[h] = part
        return 0

    lax.fori_loop(0, head_count, local_head, 0)

    def blocks(got, b, h):
        first_item = (b * head_count + h) * pick_count
        return jnp.concatenate([got[spots_smem[0, 0, first_item + k]] for k in range(pick_count)], axis=0)

    everyone = pl.ds(0, peers * cap)
    remote(k_send.at[everyone], k_got.at[everyone], 3, following).wait()

    def memory_weights(h, _):
        mix = mix_of(h)[:, :1]
        for b in range(query_count):
            raw = across(q_buf[places(b, h)], blocks(k_got, b, h))
            weights = softmax(raw, scale)
            weights_buf[b * head_count + h] = weights.astype(jnp.bfloat16)
            mixed_buf[b * head_count + h] = weights * mix
        return 0

    lax.fori_loop(0, head_count, memory_weights, 0)

    remote(v_send.at[everyone], v_got.at[everyone], 4, following).wait()

    def memory_result(step, _):
        for h in (step * 2, step * 2 + 1):
            mix = mix_of(h)
            part = gate_part[h]
            for b in range(query_count):
                at = places(b, h)
                result = onto(weights_buf[b * head_count + h], blocks(v_got, b, h))
                att_ref[at] = (mix * result + local_out[at]).astype(jnp.bfloat16)
                part = part + jnp.sum(
                    g_buf[at].astype(jnp.float32) * result, axis=0, keepdims=True
                )
            gate_part[h] = part
        return 0

    lax.fori_loop(0, head_count // 2, memory_result, 0)

    lane_ids = lax.broadcasted_iota(jnp.int32, (1, dim), 1)
    total = jnp.zeros((1, dim), jnp.float32)
    for h in range(head_count):
        mix = mix_of(h)
        term = jnp.sum(gate_part[h], axis=-1, keepdims=True) * (mix * (1.0 - mix))
        total = jnp.where(lane_ids == h, term, total)
    gate_send[...] = total
    gate_got[me] = total

    def memory_grad(step, _):
        for h in (step * 2, step * 2 + 1):
            less = 1.0 + jnp.exp(-jnp.full((1, 1), gate_ref[h], jnp.float32))
            for b in range(query_count):
                at = places(b, h)
                mixed = mixed_buf[b * head_count + h]
                weight_grad = across(g_buf[at], blocks(v_got, b, h))
                inner = jnp.sum(mixed * weight_grad, axis=-1, keepdims=True) * less
                score_grad = (mixed * (weight_grad - inner)).astype(jnp.bfloat16)
                grad = onto(score_grad, blocks(k_got, b, h))
                qg_ref[at] = ((grad + local_grad[at]) * scale).astype(jnp.bfloat16)
        return 0

    def send_gate(step, _):
        device = peer_of(step, me, mem_count)
        remote(gate_send, gate_got.at[me], 5, device).start()
        return 0

    lax.fori_loop(1, mem_count, send_gate, 0)
    lax.fori_loop(0, head_count // 2, memory_grad, 0)

    arrived = remote(gate_got.at[some], gate_got.at[some], 5, following)
    arrived.wait()
    gate_out_ref[...] = jnp.sum(gate_got[...], axis=0)


def publish(att_ref, qg_ref, gate_ref, att_hbm, qg_hbm, gate_out, sems):
    copies = [
        pltpu.make_async_copy(att_ref, att_hbm, sems.at[0]),
        pltpu.make_async_copy(qg_ref, qg_hbm, sems.at[1]),
    ]
    for copy in copies:
        copy.start()
    gate_out[...] = gate_ref[0, : gate_out.shape[0]]
    for copy in copies:
        copy.wait()


def local(
    queries,
    grad_out,
    mem_keys,
    mem_values,
    prev_keys,
    prev_values,
    gate_logit,
    location,
    top_blocks,
    write_slot,
):
    mem_count = lax.axis_size("mem")
    query_count, head_count, pick_count = top_blocks.shape
    stored, block_rows, row_width = mem_keys.shape
    dim = row_width // head_count
    cap = 2
    table_rows = stored + query_count
    any_space = pl.BlockSpec(memory_space=pl.ANY)
    smem = pl.BlockSpec(memory_space=pltpu.SMEM)
    vmem = pl.BlockSpec(memory_space=pltpu.VMEM)
    items = mem_count * cap
    weights_shape = (query_count * head_count, block_rows, pick_count * block_rows)
    attended, query_grad, gate = pl.pallas_call(
        functools.partial(kernel, mem_count, head_count, pick_count),
        out_shape=(
            pltpu.VMEM(queries.shape, jnp.bfloat16),
            pltpu.VMEM(queries.shape, jnp.bfloat16),
            pltpu.VMEM((1, dim), jnp.float32),
        ),
        in_specs=[any_space] * 6 + [smem] * 4,
        out_specs=(vmem, vmem, vmem),
        scratch_shapes=[
            pltpu.VMEM(queries.shape, jnp.bfloat16),
            pltpu.VMEM(queries.shape, jnp.bfloat16),
            pltpu.VMEM((head_count * table_rows, block_rows, dim), jnp.bfloat16),
            pltpu.VMEM((head_count * table_rows, block_rows, dim), jnp.bfloat16),
            pltpu.VMEM((2, block_rows, row_width), jnp.bfloat16),
            pltpu.VMEM((items, block_rows, dim), jnp.bfloat16),
            pltpu.VMEM((items, block_rows, dim), jnp.bfloat16),
            pltpu.VMEM((items, block_rows, dim), jnp.bfloat16),
            pltpu.VMEM((items, block_rows, dim), jnp.bfloat16),
            pltpu.VMEM((mem_count, 1, dim), jnp.int32),
            pltpu.VMEM((mem_count, 1, dim), jnp.int32),
            pltpu.SMEM((mem_count, 1, dim), jnp.int32),
            pltpu.VMEM((2, 1, dim), jnp.int32),
            pltpu.SMEM((2, 1, dim), jnp.int32),
            pltpu.VMEM(queries.shape, jnp.float32),
            pltpu.VMEM(queries.shape, jnp.float32),
            pltpu.VMEM(weights_shape, jnp.bfloat16),
            pltpu.VMEM(weights_shape, jnp.float32),
            pltpu.VMEM((head_count, 1, dim), jnp.float32),
            pltpu.VMEM((1, dim), jnp.float32),
            pltpu.VMEM((mem_count, 1, dim), jnp.float32),
            pltpu.SemaphoreType.DMA((8,)),
            pltpu.SemaphoreType.DMA((6,)),
            pltpu.SemaphoreType.DMA((6,)),
        ],
        compiler_params=pltpu.CompilerParams(
            collective_id=0, has_side_effects=True, vmem_limit_bytes=60 * 2**20
        ),
        name="retrieve_attend",
    )(
        queries,
        grad_out,
        mem_keys,
        mem_values,
        prev_keys,
        prev_values,
        jnp.transpose(top_blocks, (0, 2, 1)),
        location,
        write_slot,
        gate_logit,
    )
    return pl.pallas_call(
        publish,
        out_shape=(
            jax.ShapeDtypeStruct(queries.shape, jnp.bfloat16),
            jax.ShapeDtypeStruct(queries.shape, jnp.bfloat16),
            jax.ShapeDtypeStruct((head_count,), jnp.float32),
        ),
        in_specs=[vmem] * 3,
        out_specs=(any_space, any_space, vmem),
        scratch_shapes=[pltpu.SemaphoreType.DMA((2,))],
        name="publish",
    )(*(pltpu.with_memory_space_constraint(x, pltpu.VMEM) for x in (attended, query_grad, gate)))


def solution(mesh):
    in_specs = (
        P(("doc", "mem"), None),
        P(("doc", "mem"), None),
        P(("doc", "mem"), None, None),
        P(("doc", "mem"), None, None),
        P(("doc", "mem"), None, None),
        P(("doc", "mem"), None, None),
        P(),
        P("doc"),
        P(("doc", "mem"), None, None),
        P(("doc", "mem")),
    )
    out_specs = (P(("doc", "mem"), None), P(("doc", "mem"), None), P("doc"))
    return jax.shard_map(local, mesh=mesh, in_specs=in_specs, out_specs=out_specs, check_vma=False)
```

```python
import functools

import jax
import jax.numpy as jnp
from jax import lax
from jax.experimental import pallas as pl
from jax.experimental.pallas import tpu as pltpu
from jax.sharding import PartitionSpec as P

MESH = pl.DeviceIdType.MESH
Z_CHIPS = 8
CORES = 2
LOG2_E = 1.4426950408889634


def route(top_ref, location_ref, write_ref, mem_count, head_count, stored, cap):
    query_count, pick_count, _ = top_ref.shape
    items = query_count * head_count * pick_count
    lane = lax.broadcasted_iota(jnp.int32, (1, items), 1)

    def slots_of(h, slots):
        for b in range(query_count):
            for k in range(pick_count):
                item = (b * head_count + h) * pick_count + k
                slots = jnp.where(lane == item, location_ref[top_ref[b, k, h]], slots)
        return slots

    slots = lax.fori_loop(0, head_count, slots_of, jnp.zeros((1, items), jnp.int32))

    def split(value):
        quotient = lax.shift_right_logical(value * ((1 << 18) // stored + 1), 18)
        return quotient, value - quotient * stored

    owners, inside = split(slots)
    heads = lax.shift_right_logical(lane, pick_count.bit_length() - 1) & (head_count - 1)
    codes = heads * stored + inside
    pairs = slots * head_count + heads
    square = (items, items)
    pair_row = jnp.broadcast_to(pairs, square)
    owner_row = jnp.broadcast_to(owners, square)
    same_pair = pair_row == pair_row.T
    same_owner = owner_row == owner_row.T
    row = lax.broadcasted_iota(jnp.int32, square, 0)
    column = lax.broadcasted_iota(jnp.int32, square, 1)

    def count(condition, axis):
        return jnp.sum(jnp.where(condition, 1, 0), axis=axis, keepdims=True)

    lead_of_row = count(same_pair & (column < row), 1) == 0
    lead_of_column = count(same_pair & (row < column), 0) == 0
    rank_of_row = count(same_owner & (column < row) & lead_of_column, 1)
    position = jnp.sum(
        jnp.where(same_pair & lead_of_row, rank_of_row, 0), axis=0, keepdims=True
    )
    asked_shape = (mem_count, items)
    owner = lax.broadcasted_iota(jnp.int32, asked_shape, 0)
    asked_lane = lax.broadcasted_iota(jnp.int32, asked_shape, 1)
    asked = jnp.zeros(asked_shape, jnp.int32)
    for rank in range(cap):
        match = (owners == owner) & lead_of_column & (position == rank)
        code = jnp.sum(jnp.where(match, codes, 0), axis=1, keepdims=True)
        asked = jnp.where(asked_lane == rank, code, asked)
    head, slot = split(lane)
    place = slot
    for i in range(query_count):
        place = jnp.where(slot == write_ref[i], stored + i, place)
    return asked, owners * cap + position, head * (stored + query_count) + place


def peer_of(step, me, mem_count):
    y_chips = mem_count // (Z_CHIPS * CORES)
    y, z, c = me // (Z_CHIPS * CORES), lax.rem(me // CORES, Z_CHIPS), lax.rem(me, CORES)
    turn = step // Z_CHIPS
    place = lax.rem(step + Z_CHIPS - 1, Z_CHIPS)
    dz = Z_CHIPS // 2 + ((place + 1) // 2) * (1 - 2 * lax.rem(place, 2))
    dy = lax.rem(turn // CORES + 2 * y_chips - dz, y_chips)
    dc = lax.rem(turn, CORES)
    return (lax.rem(y + dy, y_chips) * Z_CHIPS + lax.rem(z + dz, Z_CHIPS)) * CORES + lax.rem(
        c + dc, CORES
    )


def far_first(mem_count, visit):
    turns = mem_count // Z_CHIPS

    def group(places, first_turn):
        def body(turn, _):
            for place in places:
                visit(turn * Z_CHIPS + place + 1)
            return 0

        lax.fori_loop(first_turn, turns, body, 0)

    group((0, 1, 2), 0)
    group((3, 4), 0)
    group((5, 6), 0)
    group((-1,), 1)


def across(a, b):
    return lax.dot_general(a, b, (((1,), (1,)), ((), ())), preferred_element_type=jnp.float32)


def onto(a, b):
    return lax.dot_general(a, b, (((1,), (0,)), ((), ())), preferred_element_type=jnp.float32)


def softmax(raw, scale):
    highest = jnp.max(raw, axis=-1, keepdims=True)
    expanded = jnp.exp2((raw - highest) * (scale * LOG2_E))
    return expanded * (1.0 / jnp.sum(expanded, axis=-1, keepdims=True))


def kernel(
    mem_count,
    head_count,
    pick_count,
    q_hbm,
    g_hbm,
    mk_hbm,
    mv_hbm,
    pk_hbm,
    pv_hbm,
    top_ref,
    location_ref,
    write_ref,
    gate_ref,
    att_ref,
    qg_ref,
    gate_out_ref,
    q_buf,
    g_buf,
    k_table,
    v_table,
    halo,
    k_send,
    v_send,
    k_got,
    v_got,
    codes_ref,
    code_got,
    code_smem,
    spots,
    spots_smem,
    local_out,
    local_grad,
    weights_buf,
    mixed_buf,
    gate_part,
    gate_send,
    gate_got,
    load_sems,
    send_sems,
    recv_sems,
):
    me = lax.axis_index("mem")
    stored, rows, width = mk_hbm.shape
    query_count = pk_hbm.shape[0]
    dim = width // head_count
    scale = dim**-0.5
    cap = 2
    peers = mem_count - 1

    barrier = pltpu.get_barrier_semaphore()

    def greet(step):
        pl.semaphore_signal(
            barrier, inc=1, device_id={"mem": peer_of(step, me, mem_count)}, device_id_type=MESH
        )

    far_first(mem_count, greet)

    table_rows = stored + query_count

    def load_table(source, table, offset, which):
        count = source.shape[0]

        def body(h, _):
            pltpu.make_async_copy(
                source.at[:, :, pl.ds(pl.multiple_of(h * dim, dim), dim)],
                table.at[pl.ds(h * table_rows + offset, count)],
                load_sems.at[which],
            ).start()
            return 0

        lax.fori_loop(0, head_count, body, 0)

    def await_table(source, table, which):
        whole = table.at[pl.ds(0, head_count * source.shape[0])]
        pltpu.make_async_copy(whole, whole, load_sems.at[which]).wait()

    load_table(mk_hbm, k_table, 0, 0)
    load_table(pk_hbm, k_table, stored, 1)
    load_table(mv_hbm, v_table, 0, 2)
    load_table(pv_hbm, v_table, stored, 3)
    loads = [
        pltpu.make_async_copy(q_hbm, q_buf, load_sems.at[4]),
        pltpu.make_async_copy(g_hbm, g_buf, load_sems.at[5]),
    ]
    for load in loads:
        load.start()
    asked, where, place = route(
        top_ref, location_ref, write_ref, mem_count, head_count, stored, cap
    )
    for device in range(mem_count):
        codes_ref[device] = asked[device : device + 1, :]
    spots[0] = where
    spots[1] = place
    code_got[me] = codes_ref[me]

    pl.semaphore_wait(barrier, peers)

    def remote(src, dst, which, device):
        return pltpu.make_async_remote_copy(
            src_ref=src,
            dst_ref=dst,
            send_sem=send_sems.at[which],
            recv_sem=recv_sems.at[which],
            device_id={"mem": device},
            device_id_type=MESH,
        )

    def send_codes(step):
        device = peer_of(step, me, mem_count)
        remote(codes_ref.at[device], code_got.at[me], 0, device).start()

    far_first(mem_count, send_codes)
    spots_copy = pltpu.make_async_copy(spots, spots_smem, load_sems.at[7])
    spots_copy.start()

    following = lax.rem(me + 1, mem_count)
    halo_k = remote(pk_hbm.at[query_count - 1], halo.at[0], 1, following)
    halo_v = remote(pv_hbm.at[query_count - 1], halo.at[1], 2, following)
    halo_k.start()
    halo_v.start()

    some = pl.ds(0, peers)
    remote(codes_ref.at[some], code_got.at[some], 0, following).wait()
    code_copy = pltpu.make_async_copy(code_got, code_smem, load_sems.at[6])
    code_copy.start()
    await_table(mk_hbm, k_table, 0)
    await_table(pk_hbm, k_table, 1)
    await_table(mv_hbm, v_table, 2)
    await_table(pv_hbm, v_table, 3)
    code_copy.wait()
    spots_copy.wait()

    def gather(table, device, out, at):
        for rank in range(cap):
            out[at + rank] = table[spots_smem[1, 0, code_smem[device, 0, rank]]]

    def serve(table, out, got, which):
        gather(table, peer_of(1, me, mem_count), out, cap)

        def send(step):
            device = peer_of(step, me, mem_count)
            remote(
                out.at[pl.ds(step * cap, cap)], got.at[pl.ds(me * cap, cap)], which, device
            ).start()

        def body(step, _):
            gather(table, peer_of(step, me, mem_count), out, step * cap)
            send(step - 1)
            return 0

        lax.fori_loop(2, mem_count, body, 0)
        gather(table, me, got, me * cap)
        send(peers)

    serve(k_table, k_send, k_got, 3)
    serve(v_table, v_send, v_got, 4)

    for load in loads:
        load.wait()
    halo_k.wait()
    halo_v.wait()

    first = me == 0

    def places(b, h):
        return pl.ds(b * rows, rows), pl.ds(pl.multiple_of(h * dim, dim), dim)

    def mix_of(h):
        return 1.0 / (1.0 + jnp.exp(-jnp.full((1, dim), gate_ref[h], jnp.float32)))

    def local_head(h, _):
        columns = pl.ds(pl.multiple_of(h * dim, dim), dim)
        own = h * table_rows + stored
        rest = 1.0 - mix_of(h)
        part = jnp.zeros((1, dim), jnp.float32)
        for b in range(query_count):
            at = places(b, h)
            q, g = q_buf[at], g_buf[at]
            if b == 0:
                older_k, older_v = halo[0, :, columns], halo[1, :, columns]
            else:
                older_k, older_v = k_table[own + b - 1], v_table[own + b - 1]
            keys = jnp.concatenate([older_k, k_table[own + b]], axis=0)
            values = jnp.concatenate([older_v, v_table[own + b]], axis=0)
            raw = across(q, keys)
            if b == 0:
                column_ids = lax.broadcasted_iota(jnp.int32, raw.shape, 1)
                raw = jnp.where(first & (column_ids < rows), -jnp.inf, raw)
            weights = softmax(raw, scale)
            result = onto(weights.astype(jnp.bfloat16), values)
            weight_grad = across(g, values)
            inner = jnp.sum(weights * weight_grad, axis=-1, keepdims=True)
            score_grad = weights * (weight_grad - inner) * rest[:, :1]
            local_grad[at] = onto(score_grad.astype(jnp.bfloat16), keys)
            local_out[at] = result * rest
            part = part - jnp.sum(g.astype(jnp.float32) * result, axis=0, keepdims=True)
        gate_part[h] = part
        return 0

    lax.fori_loop(0, head_count, local_head, 0)

    def blocks(got, b, h):
        first_item = (b * head_count + h) * pick_count
        return jnp.concatenate([got[spots_smem[0, 0, first_item + k]] for k in range(pick_count)], axis=0)

    everyone = pl.ds(0, peers * cap)
    remote(k_send.at[everyone], k_got.at[everyone], 3, following).wait()

    def memory_weights(h, _):
        mix = mix_of(h)[:, :1]
        for b in range(query_count):
            raw = across(q_buf[places(b, h)], blocks(k_got, b, h))
            weights = softmax(raw, scale)
            weights_buf[b * head_count + h] = weights.astype(jnp.bfloat16)
            mixed_buf[b * head_count + h] = weights * mix
        return 0

    lax.fori_loop(0, head_count, memory_weights, 0)

    remote(v_send.at[everyone], v_got.at[everyone], 4, following).wait()

    def memory_result(step, _):
        for h in (step * 2, step * 2 + 1):
            mix = mix_of(h)
            part = gate_part[h]
            for b in range(query_count):
                at = places(b, h)
                result = onto(weights_buf[b * head_count + h], blocks(v_got, b, h))
                att_ref[at] = (mix * result + local_out[at]).astype(jnp.bfloat16)
                part = part + jnp.sum(
                    g_buf[at].astype(jnp.float32) * result, axis=0, keepdims=True
                )
            gate_part[h] = part
        return 0

    lax.fori_loop(0, head_count // 2, memory_result, 0)

    lane_ids = lax.broadcasted_iota(jnp.int32, (1, dim), 1)
    total = jnp.zeros((1, dim), jnp.float32)
    for h in range(head_count):
        mix = mix_of(h)
        term = jnp.sum(gate_part[h], axis=-1, keepdims=True) * (mix * (1.0 - mix))
        total = jnp.where(lane_ids == h, term, total)
    gate_send[...] = total
    gate_got[me] = total

    def memory_grad(step, _):
        for h in (step * 2, step * 2 + 1):
            less = 1.0 + jnp.exp(-jnp.full((1, 1), gate_ref[h], jnp.float32))
            for b in range(query_count):
                at = places(b, h)
                mixed = mixed_buf[b * head_count + h]
                weight_grad = across(g_buf[at], blocks(v_got, b, h))
                inner = jnp.sum(mixed * weight_grad, axis=-1, keepdims=True) * less
                score_grad = (mixed * (weight_grad - inner)).astype(jnp.bfloat16)
                grad = onto(score_grad, blocks(k_got, b, h))
                qg_ref[at] = ((grad + local_grad[at]) * scale).astype(jnp.bfloat16)
        return 0

    def send_gate(step):
        device = peer_of(step, me, mem_count)
        remote(gate_send, gate_got.at[me], 5, device).start()

    far_first(mem_count, send_gate)
    lax.fori_loop(0, head_count // 2, memory_grad, 0)

    arrived = remote(gate_got.at[some], gate_got.at[some], 5, following)
    arrived.wait()
    gate_out_ref[...] = jnp.sum(gate_got[...], axis=0)


def publish(att_ref, qg_ref, gate_ref, att_hbm, qg_hbm, gate_out, sems):
    copies = [
        pltpu.make_async_copy(att_ref, att_hbm, sems.at[0]),
        pltpu.make_async_copy(qg_ref, qg_hbm, sems.at[1]),
    ]
    for copy in copies:
        copy.start()
    gate_out[...] = gate_ref[0, : gate_out.shape[0]]
    for copy in copies:
        copy.wait()


def local(
    queries,
    grad_out,
    mem_keys,
    mem_values,
    prev_keys,
    prev_values,
    gate_logit,
    location,
    top_blocks,
    write_slot,
):
    mem_count = lax.axis_size("mem")
    query_count, head_count, pick_count = top_blocks.shape
    stored, block_rows, row_width = mem_keys.shape
    dim = row_width // head_count
    cap = 2
    table_rows = stored + query_count
    any_space = pl.BlockSpec(memory_space=pl.ANY)
    smem = pl.BlockSpec(memory_space=pltpu.SMEM)
    vmem = pl.BlockSpec(memory_space=pltpu.VMEM)
    items = mem_count * cap
    weights_shape = (query_count * head_count, block_rows, pick_count * block_rows)
    attended, query_grad, gate = pl.pallas_call(
        functools.partial(kernel, mem_count, head_count, pick_count),
        out_shape=(
            pltpu.VMEM(queries.shape, jnp.bfloat16),
            pltpu.VMEM(queries.shape, jnp.bfloat16),
            pltpu.VMEM((1, dim), jnp.float32),
        ),
        in_specs=[any_space] * 6 + [smem] * 4,
        out_specs=(vmem, vmem, vmem),
        scratch_shapes=[
            pltpu.VMEM(queries.shape, jnp.bfloat16),
            pltpu.VMEM(queries.shape, jnp.bfloat16),
            pltpu.VMEM((head_count * table_rows, block_rows, dim), jnp.bfloat16),
            pltpu.VMEM((head_count * table_rows, block_rows, dim), jnp.bfloat16),
            pltpu.VMEM((2, block_rows, row_width), jnp.bfloat16),
            pltpu.VMEM((items, block_rows, dim), jnp.bfloat16),
            pltpu.VMEM((items, block_rows, dim), jnp.bfloat16),
            pltpu.VMEM((items, block_rows, dim), jnp.bfloat16),
            pltpu.VMEM((items, block_rows, dim), jnp.bfloat16),
            pltpu.VMEM((mem_count, 1, dim), jnp.int32),
            pltpu.VMEM((mem_count, 1, dim), jnp.int32),
            pltpu.SMEM((mem_count, 1, dim), jnp.int32),
            pltpu.VMEM((2, 1, dim), jnp.int32),
            pltpu.SMEM((2, 1, dim), jnp.int32),
            pltpu.VMEM(queries.shape, jnp.float32),
            pltpu.VMEM(queries.shape, jnp.float32),
            pltpu.VMEM(weights_shape, jnp.bfloat16),
            pltpu.VMEM(weights_shape, jnp.float32),
            pltpu.VMEM((head_count, 1, dim), jnp.float32),
            pltpu.VMEM((1, dim), jnp.float32),
            pltpu.VMEM((mem_count, 1, dim), jnp.float32),
            pltpu.SemaphoreType.DMA((8,)),
            pltpu.SemaphoreType.DMA((6,)),
            pltpu.SemaphoreType.DMA((6,)),
        ],
        compiler_params=pltpu.CompilerParams(
            collective_id=0, has_side_effects=True, vmem_limit_bytes=60 * 2**20
        ),
        name="retrieve_attend",
    )(
        queries,
        grad_out,
        mem_keys,
        mem_values,
        prev_keys,
        prev_values,
        jnp.transpose(top_blocks, (0, 2, 1)),
        location,
        write_slot,
        gate_logit,
    )
    return pl.pallas_call(
        publish,
        out_shape=(
            jax.ShapeDtypeStruct(queries.shape, jnp.bfloat16),
            jax.ShapeDtypeStruct(queries.shape, jnp.bfloat16),
            jax.ShapeDtypeStruct((head_count,), jnp.float32),
        ),
        in_specs=[vmem] * 3,
        out_specs=(any_space, any_space, vmem),
        scratch_shapes=[pltpu.SemaphoreType.DMA((2,))],
        name="publish",
    )(*(pltpu.with_memory_space_constraint(x, pltpu.VMEM) for x in (attended, query_grad, gate)))


def solution(mesh):
    in_specs = (
        P(("doc", "mem"), None),
        P(("doc", "mem"), None),
        P(("doc", "mem"), None, None),
        P(("doc", "mem"), None, None),
        P(("doc", "mem"), None, None),
        P(("doc", "mem"), None, None),
        P(),
        P("doc"),
        P(("doc", "mem"), None, None),
        P(("doc", "mem")),
    )
    out_specs = (P(("doc", "mem"), None), P(("doc", "mem"), None), P("doc"))
    return jax.shard_map(local, mesh=mesh, in_specs=in_specs, out_specs=out_specs, check_vma=False)
```

```python
import functools

import jax
import jax.numpy as jnp
from jax import lax
from jax.experimental import pallas as pl
from jax.experimental.pallas import tpu as pltpu
from jax.sharding import PartitionSpec as P

MESH = pl.DeviceIdType.MESH
Z_CHIPS = 8
CORES = 2
LOG2_E = 1.4426950408889634


def route(top_ref, location_ref, write_ref, mem_count, head_count, stored, cap):
    query_count, pick_count, _ = top_ref.shape
    items = query_count * head_count * pick_count
    lane = lax.broadcasted_iota(jnp.int32, (1, items), 1)

    def slots_of(h, slots):
        for b in range(query_count):
            for k in range(pick_count):
                item = (b * head_count + h) * pick_count + k
                slots = jnp.where(lane == item, location_ref[top_ref[b, k, h]], slots)
        return slots

    slots = lax.fori_loop(0, head_count, slots_of, jnp.zeros((1, items), jnp.int32))

    def split(value):
        quotient = lax.shift_right_logical(value * ((1 << 18) // stored + 1), 18)
        return quotient, value - quotient * stored

    owners, inside = split(slots)
    heads = lax.shift_right_logical(lane, pick_count.bit_length() - 1) & (head_count - 1)
    codes = heads * stored + inside
    pairs = slots * head_count + heads
    square = (items, items)
    pair_row = jnp.broadcast_to(pairs, square)
    owner_row = jnp.broadcast_to(owners, square)
    same_pair = pair_row == pair_row.T
    same_owner = owner_row == owner_row.T
    row = lax.broadcasted_iota(jnp.int32, square, 0)
    column = lax.broadcasted_iota(jnp.int32, square, 1)

    def count(condition, axis):
        return jnp.sum(jnp.where(condition, 1, 0), axis=axis, keepdims=True)

    lead_of_row = count(same_pair & (column < row), 1) == 0
    lead_of_column = count(same_pair & (row < column), 0) == 0
    rank_of_row = count(same_owner & (column < row) & lead_of_column, 1)
    position = jnp.sum(
        jnp.where(same_pair & lead_of_row, rank_of_row, 0), axis=0, keepdims=True
    )
    asked_shape = (mem_count, items)
    owner = lax.broadcasted_iota(jnp.int32, asked_shape, 0)
    asked_lane = lax.broadcasted_iota(jnp.int32, asked_shape, 1)
    asked = jnp.zeros(asked_shape, jnp.int32)
    for rank in range(cap):
        match = (owners == owner) & lead_of_column & (position == rank)
        code = jnp.sum(jnp.where(match, codes, 0), axis=1, keepdims=True)
        asked = jnp.where(asked_lane == rank, code, asked)
    head, slot = split(lane)
    place = slot
    for i in range(query_count):
        place = jnp.where(slot == write_ref[i], stored + i, place)
    return asked, owners * cap + position, head * (stored + query_count) + place


def peer_of(step, me, mem_count):
    y_chips = mem_count // (Z_CHIPS * CORES)
    y, z, c = me // (Z_CHIPS * CORES), lax.rem(me // CORES, Z_CHIPS), lax.rem(me, CORES)
    turn = step // Z_CHIPS
    place = lax.rem(step + Z_CHIPS - 1, Z_CHIPS)
    dz = Z_CHIPS // 2 + ((place + 1) // 2) * (1 - 2 * lax.rem(place, 2))
    dy = lax.rem(turn // CORES + 2 * y_chips - dz, y_chips)
    dc = lax.rem(turn, CORES)
    return (lax.rem(y + dy, y_chips) * Z_CHIPS + lax.rem(z + dz, Z_CHIPS)) * CORES + lax.rem(
        c + dc, CORES
    )


def far_first(mem_count, visit):
    turns = mem_count // Z_CHIPS

    def group(places, first_turn):
        def body(turn, _):
            for place in places:
                visit(turn * Z_CHIPS + place + 1)
            return 0

        lax.fori_loop(first_turn, turns, body, 0)

    group((0, 1, 2), 0)
    group((3, 4), 0)
    group((5, 6), 0)
    group((-1,), 1)


def across(a, b):
    return lax.dot_general(a, b, (((1,), (1,)), ((), ())), preferred_element_type=jnp.float32)


def onto(a, b):
    return lax.dot_general(a, b, (((1,), (0,)), ((), ())), preferred_element_type=jnp.float32)


def softmax(raw, scale):
    highest = jnp.max(raw, axis=-1, keepdims=True)
    expanded = jnp.exp2((raw - highest) * (scale * LOG2_E))
    return expanded * (1.0 / jnp.sum(expanded, axis=-1, keepdims=True))


def kernel(
    mem_count,
    head_count,
    pick_count,
    q_hbm,
    g_hbm,
    mk_hbm,
    mv_hbm,
    pk_hbm,
    pv_hbm,
    top_ref,
    location_ref,
    write_ref,
    gate_ref,
    att_ref,
    qg_ref,
    gate_out_ref,
    q_buf,
    g_buf,
    k_table,
    v_table,
    halo,
    k_send,
    v_send,
    k_got,
    v_got,
    codes_ref,
    code_got,
    code_smem,
    spots,
    spots_smem,
    local_out,
    local_grad,
    weights_buf,
    mixed_buf,
    gate_part,
    gate_send,
    gate_got,
    load_sems,
    send_sems,
    recv_sems,
):
    me = lax.axis_index("mem")
    stored, rows, width = mk_hbm.shape
    query_count = pk_hbm.shape[0]
    dim = width // head_count
    scale = dim**-0.5
    cap = 2
    peers = mem_count - 1
    together = 4

    barrier = pltpu.get_barrier_semaphore()

    def greet(step):
        pl.semaphore_signal(
            barrier, inc=1, device_id={"mem": peer_of(step, me, mem_count)}, device_id_type=MESH
        )

    far_first(mem_count, greet)

    table_rows = stored + query_count

    def load_table(source, table, offset, which):
        count = source.shape[0]

        def body(h, _):
            pltpu.make_async_copy(
                source.at[:, :, pl.ds(pl.multiple_of(h * dim, dim), dim)],
                table.at[pl.ds(h * table_rows + offset, count)],
                load_sems.at[which],
            ).start()
            return 0

        lax.fori_loop(0, head_count, body, 0)

    def await_table(source, table, which):
        whole = table.at[pl.ds(0, head_count * source.shape[0])]
        pltpu.make_async_copy(whole, whole, load_sems.at[which]).wait()

    load_table(mk_hbm, k_table, 0, 0)
    load_table(pk_hbm, k_table, stored, 1)
    asked, where, place = route(
        top_ref, location_ref, write_ref, mem_count, head_count, stored, cap
    )
    for device in range(mem_count):
        codes_ref[device] = asked[device : device + 1, :]
    spots[0] = where
    spots[1] = place
    code_got[me] = codes_ref[me]

    pl.semaphore_wait(barrier, peers)

    def remote(src, dst, which, device):
        return pltpu.make_async_remote_copy(
            src_ref=src,
            dst_ref=dst,
            send_sem=send_sems.at[which],
            recv_sem=recv_sems.at[which],
            device_id={"mem": device},
            device_id_type=MESH,
        )

    def send_codes(step):
        device = peer_of(step, me, mem_count)
        remote(codes_ref.at[device], code_got.at[me], 0, device).start()

    far_first(mem_count, send_codes)
    spots_copy = pltpu.make_async_copy(spots, spots_smem, load_sems.at[7])
    spots_copy.start()

    following = lax.rem(me + 1, mem_count)
    halo_k = remote(pk_hbm.at[query_count - 1], halo.at[0], 1, following)
    halo_v = remote(pv_hbm.at[query_count - 1], halo.at[1], 2, following)
    halo_k.start()
    halo_v.start()
    load_table(mv_hbm, v_table, 0, 2)
    load_table(pv_hbm, v_table, stored, 3)
    loads = [
        pltpu.make_async_copy(q_hbm, q_buf, load_sems.at[4]),
        pltpu.make_async_copy(g_hbm, g_buf, load_sems.at[5]),
    ]
    for load in loads:
        load.start()

    some = pl.ds(0, peers)
    remote(codes_ref.at[some], code_got.at[some], 0, following).wait()
    code_copy = pltpu.make_async_copy(code_got, code_smem, load_sems.at[6])
    code_copy.start()
    await_table(mk_hbm, k_table, 0)
    await_table(pk_hbm, k_table, 1)
    code_copy.wait()
    spots_copy.wait()

    def gather(table, device, out, at):
        for rank in range(cap):
            out[at + rank] = table[spots_smem[1, 0, code_smem[device, 0, rank]]]

    def serve(table, out, got, which):
        gather(table, peer_of(1, me, mem_count), out, cap)

        def send(step):
            device = peer_of(step, me, mem_count)
            remote(
                out.at[pl.ds(step * cap, cap)], got.at[pl.ds(me * cap, cap)], which, device
            ).start()

        def body(step, _):
            gather(table, peer_of(step, me, mem_count), out, step * cap)
            send(step - 1)
            return 0

        lax.fori_loop(2, mem_count, body, 0)
        gather(table, me, got, me * cap)
        send(peers)

    serve(k_table, k_send, k_got, 3)
    await_table(mv_hbm, v_table, 2)
    await_table(pv_hbm, v_table, 3)
    serve(v_table, v_send, v_got, 4)

    for load in loads:
        load.wait()
    halo_k.wait()
    halo_v.wait()

    first = me == 0

    def places(b, h):
        return pl.ds(b * rows, rows), pl.ds(pl.multiple_of(h * dim, dim), dim)

    def mix_of(h):
        return 1.0 / (1.0 + jnp.exp(-jnp.full((1, dim), gate_ref[h], jnp.float32)))

    def local_head(h, _):
        columns = pl.ds(pl.multiple_of(h * dim, dim), dim)
        own = h * table_rows + stored
        rest = 1.0 - mix_of(h)
        part = jnp.zeros((1, dim), jnp.float32)
        for b in range(query_count):
            at = places(b, h)
            q, g = q_buf[at], g_buf[at]
            if b == 0:
                older_k, older_v = halo[0, :, columns], halo[1, :, columns]
            else:
                older_k, older_v = k_table[own + b - 1], v_table[own + b - 1]
            keys = jnp.concatenate([older_k, k_table[own + b]], axis=0)
            values = jnp.concatenate([older_v, v_table[own + b]], axis=0)
            raw = across(q, keys)
            if b == 0:
                column_ids = lax.broadcasted_iota(jnp.int32, raw.shape, 1)
                raw = jnp.where(first & (column_ids < rows), -jnp.inf, raw)
            weights = softmax(raw, scale)
            result = onto(weights.astype(jnp.bfloat16), values)
            weight_grad = across(g, values)
            inner = jnp.sum(weights * weight_grad, axis=-1, keepdims=True)
            score_grad = weights * (weight_grad - inner) * rest[:, :1]
            local_grad[at] = onto(score_grad.astype(jnp.bfloat16), keys)
            local_out[at] = result * rest
            part = part - jnp.sum(g.astype(jnp.float32) * result, axis=0, keepdims=True)
        gate_part[h] = part
        return 0

    lax.fori_loop(0, head_count, local_head, 0)

    def blocks(got, b, h):
        first_item = (b * head_count + h) * pick_count
        return jnp.concatenate([got[spots_smem[0, 0, first_item + k]] for k in range(pick_count)], axis=0)

    everyone = pl.ds(0, peers * cap)
    remote(k_send.at[everyone], k_got.at[everyone], 3, following).wait()

    def memory_weights(h, _):
        mix = mix_of(h)[:, :1]
        for b in range(query_count):
            raw = across(q_buf[places(b, h)], blocks(k_got, b, h))
            weights = softmax(raw, scale)
            weights_buf[b * head_count + h] = weights.astype(jnp.bfloat16)
            mixed_buf[b * head_count + h] = weights * mix
        return 0

    lax.fori_loop(0, head_count, memory_weights, 0)

    remote(v_send.at[everyone], v_got.at[everyone], 4, following).wait()

    def memory_result(step, _):
        for h in [step * together + i for i in range(together)]:
            mix = mix_of(h)
            part = gate_part[h]
            for b in range(query_count):
                at = places(b, h)
                result = onto(weights_buf[b * head_count + h], blocks(v_got, b, h))
                att_ref[at] = (mix * result + local_out[at]).astype(jnp.bfloat16)
                part = part + jnp.sum(
                    g_buf[at].astype(jnp.float32) * result, axis=0, keepdims=True
                )
            gate_part[h] = part
        return 0

    lax.fori_loop(0, head_count // together, memory_result, 0)

    lane_ids = lax.broadcasted_iota(jnp.int32, (1, dim), 1)
    total = jnp.zeros((1, dim), jnp.float32)
    for h in range(head_count):
        mix = mix_of(h)
        term = jnp.sum(gate_part[h], axis=-1, keepdims=True) * (mix * (1.0 - mix))
        total = jnp.where(lane_ids == h, term, total)
    gate_send[...] = total
    gate_got[me] = total

    def memory_grad(step, _):
        for h in [step * together + i for i in range(together)]:
            less = 1.0 + jnp.exp(-jnp.full((1, 1), gate_ref[h], jnp.float32))
            for b in range(query_count):
                at = places(b, h)
                mixed = mixed_buf[b * head_count + h]
                weight_grad = across(g_buf[at], blocks(v_got, b, h))
                inner = jnp.sum(mixed * weight_grad, axis=-1, keepdims=True) * less
                score_grad = (mixed * (weight_grad - inner)).astype(jnp.bfloat16)
                grad = onto(score_grad, blocks(k_got, b, h))
                qg_ref[at] = ((grad + local_grad[at]) * scale).astype(jnp.bfloat16)
        return 0

    def send_gate(step):
        device = peer_of(step, me, mem_count)
        remote(gate_send, gate_got.at[me], 5, device).start()

    far_first(mem_count, send_gate)
    lax.fori_loop(0, head_count // together, memory_grad, 0)

    arrived = remote(gate_got.at[some], gate_got.at[some], 5, following)
    arrived.wait()
    gate_out_ref[...] = jnp.sum(gate_got[...], axis=0)


def publish(att_ref, qg_ref, gate_ref, att_hbm, qg_hbm, gate_out, sems):
    copies = [
        pltpu.make_async_copy(att_ref, att_hbm, sems.at[0]),
        pltpu.make_async_copy(qg_ref, qg_hbm, sems.at[1]),
    ]
    for copy in copies:
        copy.start()
    gate_out[...] = gate_ref[0, : gate_out.shape[0]]
    for copy in copies:
        copy.wait()


def local(
    queries,
    grad_out,
    mem_keys,
    mem_values,
    prev_keys,
    prev_values,
    gate_logit,
    location,
    top_blocks,
    write_slot,
):
    mem_count = lax.axis_size("mem")
    query_count, head_count, pick_count = top_blocks.shape
    stored, block_rows, row_width = mem_keys.shape
    dim = row_width // head_count
    cap = 2
    table_rows = stored + query_count
    any_space = pl.BlockSpec(memory_space=pl.ANY)
    smem = pl.BlockSpec(memory_space=pltpu.SMEM)
    vmem = pl.BlockSpec(memory_space=pltpu.VMEM)
    items = mem_count * cap
    weights_shape = (query_count * head_count, block_rows, pick_count * block_rows)
    attended, query_grad, gate = pl.pallas_call(
        functools.partial(kernel, mem_count, head_count, pick_count),
        out_shape=(
            pltpu.VMEM(queries.shape, jnp.bfloat16),
            pltpu.VMEM(queries.shape, jnp.bfloat16),
            pltpu.VMEM((1, dim), jnp.float32),
        ),
        in_specs=[any_space] * 6 + [smem] * 4,
        out_specs=(vmem, vmem, vmem),
        scratch_shapes=[
            pltpu.VMEM(queries.shape, jnp.bfloat16),
            pltpu.VMEM(queries.shape, jnp.bfloat16),
            pltpu.VMEM((head_count * table_rows, block_rows, dim), jnp.bfloat16),
            pltpu.VMEM((head_count * table_rows, block_rows, dim), jnp.bfloat16),
            pltpu.VMEM((2, block_rows, row_width), jnp.bfloat16),
            pltpu.VMEM((items, block_rows, dim), jnp.bfloat16),
            pltpu.VMEM((items, block_rows, dim), jnp.bfloat16),
            pltpu.VMEM((items, block_rows, dim), jnp.bfloat16),
            pltpu.VMEM((items, block_rows, dim), jnp.bfloat16),
            pltpu.VMEM((mem_count, 1, dim), jnp.int32),
            pltpu.VMEM((mem_count, 1, dim), jnp.int32),
            pltpu.SMEM((mem_count, 1, dim), jnp.int32),
            pltpu.VMEM((2, 1, dim), jnp.int32),
            pltpu.SMEM((2, 1, dim), jnp.int32),
            pltpu.VMEM(queries.shape, jnp.float32),
            pltpu.VMEM(queries.shape, jnp.float32),
            pltpu.VMEM(weights_shape, jnp.bfloat16),
            pltpu.VMEM(weights_shape, jnp.float32),
            pltpu.VMEM((head_count, 1, dim), jnp.float32),
            pltpu.VMEM((1, dim), jnp.float32),
            pltpu.VMEM((mem_count, 1, dim), jnp.float32),
            pltpu.SemaphoreType.DMA((8,)),
            pltpu.SemaphoreType.DMA((6,)),
            pltpu.SemaphoreType.DMA((6,)),
        ],
        compiler_params=pltpu.CompilerParams(
            collective_id=0, has_side_effects=True, vmem_limit_bytes=60 * 2**20
        ),
        name="retrieve_attend",
    )(
        queries,
        grad_out,
        mem_keys,
        mem_values,
        prev_keys,
        prev_values,
        jnp.transpose(top_blocks, (0, 2, 1)),
        location,
        write_slot,
        gate_logit,
    )
    return pl.pallas_call(
        publish,
        out_shape=(
            jax.ShapeDtypeStruct(queries.shape, jnp.bfloat16),
            jax.ShapeDtypeStruct(queries.shape, jnp.bfloat16),
            jax.ShapeDtypeStruct((head_count,), jnp.float32),
        ),
        in_specs=[vmem] * 3,
        out_specs=(any_space, any_space, vmem),
        scratch_shapes=[pltpu.SemaphoreType.DMA((2,))],
        name="publish",
    )(*(pltpu.with_memory_space_constraint(x, pltpu.VMEM) for x in (attended, query_grad, gate)))


def solution(mesh):
    in_specs = (
        P(("doc", "mem"), None),
        P(("doc", "mem"), None),
        P(("doc", "mem"), None, None),
        P(("doc", "mem"), None, None),
        P(("doc", "mem"), None, None),
        P(("doc", "mem"), None, None),
        P(),
        P("doc"),
        P(("doc", "mem"), None, None),
        P(("doc", "mem")),
    )
    out_specs = (P(("doc", "mem"), None), P(("doc", "mem"), None), P("doc"))
    return jax.shard_map(local, mesh=mesh, in_specs=in_specs, out_specs=out_specs, check_vma=False)
```

```python
import functools

import jax
import jax.numpy as jnp
from jax import lax
from jax.experimental import pallas as pl
from jax.experimental.pallas import tpu as pltpu
from jax.sharding import PartitionSpec as P

MESH = pl.DeviceIdType.MESH
Z_CHIPS = 8
CORES = 2
LOG2_E = 1.4426950408889634


def route(top_ref, location_ref, write_ref, mem_count, head_count, stored, cap):
    query_count, pick_count, _ = top_ref.shape
    items = query_count * head_count * pick_count
    lane = lax.broadcasted_iota(jnp.int32, (1, items), 1)

    def slots_of(h, slots):
        for b in range(query_count):
            for k in range(pick_count):
                item = (b * head_count + h) * pick_count + k
                slots = jnp.where(lane == item, location_ref[top_ref[b, k, h]], slots)
        return slots

    slots = lax.fori_loop(0, head_count, slots_of, jnp.zeros((1, items), jnp.int32))

    def split(value):
        quotient = lax.shift_right_logical(value * ((1 << 18) // stored + 1), 18)
        return quotient, value - quotient * stored

    owners, inside = split(slots)
    heads = lax.shift_right_logical(lane, pick_count.bit_length() - 1) & (head_count - 1)
    codes = heads * stored + inside
    pairs = slots * head_count + heads
    square = (items, items)
    pair_row = jnp.broadcast_to(pairs, square)
    owner_row = jnp.broadcast_to(owners, square)
    same_pair = pair_row == pair_row.T
    same_owner = owner_row == owner_row.T
    row = lax.broadcasted_iota(jnp.int32, square, 0)
    column = lax.broadcasted_iota(jnp.int32, square, 1)

    def count(condition, axis):
        return jnp.sum(jnp.where(condition, 1, 0), axis=axis, keepdims=True)

    lead_of_row = count(same_pair & (column < row), 1) == 0
    lead_of_column = count(same_pair & (row < column), 0) == 0
    rank_of_row = count(same_owner & (column < row) & lead_of_column, 1)
    position = jnp.sum(
        jnp.where(same_pair & lead_of_row, rank_of_row, 0), axis=0, keepdims=True
    )
    asked_shape = (mem_count, items)
    owner = lax.broadcasted_iota(jnp.int32, asked_shape, 0)
    asked_lane = lax.broadcasted_iota(jnp.int32, asked_shape, 1)
    asked = jnp.zeros(asked_shape, jnp.int32)
    for rank in range(cap):
        match = (owners == owner) & lead_of_column & (position == rank)
        code = jnp.sum(jnp.where(match, codes, 0), axis=1, keepdims=True)
        asked = jnp.where(asked_lane == rank, code, asked)
    head, slot = split(lane)
    place = slot
    for i in range(query_count):
        place = jnp.where(slot == write_ref[i], stored + i, place)
    return asked, owners * cap + position, head * (stored + query_count) + place


def peer_of(step, me, mem_count):
    y_chips = mem_count // (Z_CHIPS * CORES)
    y, z, c = me // (Z_CHIPS * CORES), lax.rem(me // CORES, Z_CHIPS), lax.rem(me, CORES)
    turn = step // Z_CHIPS
    place = lax.rem(step + Z_CHIPS - 1, Z_CHIPS)
    dz = Z_CHIPS // 2 + ((place + 1) // 2) * (1 - 2 * lax.rem(place, 2))
    dy = lax.rem(turn // CORES + 2 * y_chips - dz, y_chips)
    dc = lax.rem(turn, CORES)
    return (lax.rem(y + dy, y_chips) * Z_CHIPS + lax.rem(z + dz, Z_CHIPS)) * CORES + lax.rem(
        c + dc, CORES
    )


def far_first(mem_count, visit):
    turns = mem_count // Z_CHIPS

    def group(places, first_turn):
        def body(turn, _):
            for place in places:
                visit(turn * Z_CHIPS + place + 1)
            return 0

        lax.fori_loop(first_turn, turns, body, 0)

    group((0, 1, 2), 0)
    group((3, 4), 0)
    group((5, 6), 0)
    group((-1,), 1)


def across(a, b):
    return lax.dot_general(a, b, (((1,), (1,)), ((), ())), preferred_element_type=jnp.float32)


def onto(a, b):
    return lax.dot_general(a, b, (((1,), (0,)), ((), ())), preferred_element_type=jnp.float32)


def softmax(raw, scale):
    highest = jnp.max(raw, axis=-1, keepdims=True)
    expanded = jnp.exp2((raw - highest) * (scale * LOG2_E))
    return expanded * (1.0 / jnp.sum(expanded, axis=-1, keepdims=True))


def kernel(
    mem_count,
    head_count,
    pick_count,
    q_hbm,
    g_hbm,
    mk_hbm,
    mv_hbm,
    pk_hbm,
    pv_hbm,
    top_ref,
    location_ref,
    write_ref,
    gate_ref,
    att_ref,
    qg_ref,
    gate_out_ref,
    q_buf,
    g_buf,
    k_table,
    v_table,
    halo,
    k_send,
    v_send,
    k_got,
    v_got,
    codes_ref,
    code_got,
    code_smem,
    spots,
    spots_smem,
    local_out,
    local_grad,
    weights_buf,
    mixed_buf,
    gate_part,
    gate_send,
    gate_got,
    load_sems,
    send_sems,
    recv_sems,
):
    me = lax.axis_index("mem")
    stored, rows, width = mk_hbm.shape
    query_count = pk_hbm.shape[0]
    dim = width // head_count
    scale = dim**-0.5
    cap = 2
    peers = mem_count - 1
    together = 4

    barrier = pltpu.get_barrier_semaphore()

    def greet(step):
        pl.semaphore_signal(
            barrier, inc=1, device_id={"mem": peer_of(step, me, mem_count)}, device_id_type=MESH
        )

    far_first(mem_count, greet)

    table_rows = stored + query_count

    def load_table(source, table, offset, which):
        count = source.shape[0]

        def body(h, _):
            pltpu.make_async_copy(
                source.at[:, :, pl.ds(pl.multiple_of(h * dim, dim), dim)],
                table.at[pl.ds(h * table_rows + offset, count)],
                load_sems.at[which],
            ).start()
            return 0

        lax.fori_loop(0, head_count, body, 0)

    def await_table(source, table, which):
        whole = table.at[pl.ds(0, head_count * source.shape[0])]
        pltpu.make_async_copy(whole, whole, load_sems.at[which]).wait()

    asked, where, place = route(
        top_ref, location_ref, write_ref, mem_count, head_count, stored, cap
    )
    for device in range(mem_count):
        codes_ref[device] = asked[device : device + 1, :]
    spots[0] = where
    spots[1] = place
    code_got[me] = codes_ref[me]

    pl.semaphore_wait(barrier, peers)

    def remote(src, dst, which, device):
        return pltpu.make_async_remote_copy(
            src_ref=src,
            dst_ref=dst,
            send_sem=send_sems.at[which],
            recv_sem=recv_sems.at[which],
            device_id={"mem": device},
            device_id_type=MESH,
        )

    def send_codes(step):
        device = peer_of(step, me, mem_count)
        remote(codes_ref.at[device], code_got.at[me], 0, device).start()

    far_first(mem_count, send_codes)
    spots_copy = pltpu.make_async_copy(spots, spots_smem, load_sems.at[7])
    spots_copy.start()

    following = lax.rem(me + 1, mem_count)
    halo_k = remote(pk_hbm.at[query_count - 1], halo.at[0], 1, following)
    halo_v = remote(pv_hbm.at[query_count - 1], halo.at[1], 2, following)
    halo_k.start()
    halo_v.start()
    load_table(mk_hbm, k_table, 0, 0)
    load_table(pk_hbm, k_table, stored, 1)
    load_table(mv_hbm, v_table, 0, 2)
    load_table(pv_hbm, v_table, stored, 3)
    loads = [
        pltpu.make_async_copy(q_hbm, q_buf, load_sems.at[4]),
        pltpu.make_async_copy(g_hbm, g_buf, load_sems.at[5]),
    ]
    for load in loads:
        load.start()

    some = pl.ds(0, peers)
    remote(codes_ref.at[some], code_got.at[some], 0, following).wait()
    code_copy = pltpu.make_async_copy(code_got, code_smem, load_sems.at[6])
    code_copy.start()
    await_table(mk_hbm, k_table, 0)
    await_table(pk_hbm, k_table, 1)
    code_copy.wait()
    spots_copy.wait()

    def gather(table, device, out, at):
        for rank in range(cap):
            out[at + rank] = table[spots_smem[1, 0, code_smem[device, 0, rank]]]

    def serve(table, out, got, which):
        gather(table, peer_of(1, me, mem_count), out, cap)

        def send(step):
            device = peer_of(step, me, mem_count)
            remote(
                out.at[pl.ds(step * cap, cap)], got.at[pl.ds(me * cap, cap)], which, device
            ).start()

        def body(step, _):
            gather(table, peer_of(step, me, mem_count), out, step * cap)
            send(step - 1)
            return 0

        lax.fori_loop(2, mem_count, body, 0)
        gather(table, me, got, me * cap)
        send(peers)

    serve(k_table, k_send, k_got, 3)
    await_table(mv_hbm, v_table, 2)
    await_table(pv_hbm, v_table, 3)
    serve(v_table, v_send, v_got, 4)

    for load in loads:
        load.wait()
    halo_k.wait()
    halo_v.wait()

    first = me == 0

    def places(b, h):
        return pl.ds(b * rows, rows), pl.ds(pl.multiple_of(h * dim, dim), dim)

    def mix_of(h):
        return 1.0 / (1.0 + jnp.exp(-jnp.full((1, dim), gate_ref[h], jnp.float32)))

    def local_head(h, _):
        columns = pl.ds(pl.multiple_of(h * dim, dim), dim)
        own = h * table_rows + stored
        rest = 1.0 - mix_of(h)
        part = jnp.zeros((1, dim), jnp.float32)
        for b in range(query_count):
            at = places(b, h)
            q, g = q_buf[at], g_buf[at]
            if b == 0:
                older_k, older_v = halo[0, :, columns], halo[1, :, columns]
            else:
                older_k, older_v = k_table[own + b - 1], v_table[own + b - 1]
            keys = jnp.concatenate([older_k, k_table[own + b]], axis=0)
            values = jnp.concatenate([older_v, v_table[own + b]], axis=0)
            raw = across(q, keys)
            if b == 0:
                column_ids = lax.broadcasted_iota(jnp.int32, raw.shape, 1)
                raw = jnp.where(first & (column_ids < rows), -jnp.inf, raw)
            weights = softmax(raw, scale)
            result = onto(weights.astype(jnp.bfloat16), values)
            weight_grad = across(g, values)
            inner = jnp.sum(weights * weight_grad, axis=-1, keepdims=True)
            score_grad = weights * (weight_grad - inner) * rest[:, :1]
            local_grad[at] = onto(score_grad.astype(jnp.bfloat16), keys)
            local_out[at] = result * rest
            part = part - jnp.sum(g.astype(jnp.float32) * result, axis=0, keepdims=True)
        gate_part[h] = part
        return 0

    lax.fori_loop(0, head_count, local_head, 0)

    def blocks(got, b, h):
        first_item = (b * head_count + h) * pick_count
        return jnp.concatenate([got[spots_smem[0, 0, first_item + k]] for k in range(pick_count)], axis=0)

    everyone = pl.ds(0, peers * cap)
    remote(k_send.at[everyone], k_got.at[everyone], 3, following).wait()

    def memory_weights(h, _):
        mix = mix_of(h)[:, :1]
        for b in range(query_count):
            raw = across(q_buf[places(b, h)], blocks(k_got, b, h))
            weights = softmax(raw, scale)
            weights_buf[b * head_count + h] = weights.astype(jnp.bfloat16)
            mixed_buf[b * head_count + h] = weights * mix
        return 0

    lax.fori_loop(0, head_count, memory_weights, 0)

    remote(v_send.at[everyone], v_got.at[everyone], 4, following).wait()

    def memory_result(step, _):
        for h in [step * together + i for i in range(together)]:
            mix = mix_of(h)
            part = gate_part[h]
            for b in range(query_count):
                at = places(b, h)
                result = onto(weights_buf[b * head_count + h], blocks(v_got, b, h))
                att_ref[at] = (mix * result + local_out[at]).astype(jnp.bfloat16)
                part = part + jnp.sum(
                    g_buf[at].astype(jnp.float32) * result, axis=0, keepdims=True
                )
            gate_part[h] = part
        return 0

    lax.fori_loop(0, head_count // together, memory_result, 0)

    lane_ids = lax.broadcasted_iota(jnp.int32, (1, dim), 1)
    total = jnp.zeros((1, dim), jnp.float32)
    for h in range(head_count):
        mix = mix_of(h)
        term = jnp.sum(gate_part[h], axis=-1, keepdims=True) * (mix * (1.0 - mix))
        total = jnp.where(lane_ids == h, term, total)
    gate_send[...] = total
    gate_got[me] = total

    def memory_grad(step, _):
        for h in [step * together + i for i in range(together)]:
            less = 1.0 + jnp.exp(-jnp.full((1, 1), gate_ref[h], jnp.float32))
            for b in range(query_count):
                at = places(b, h)
                mixed = mixed_buf[b * head_count + h]
                weight_grad = across(g_buf[at], blocks(v_got, b, h))
                inner = jnp.sum(mixed * weight_grad, axis=-1, keepdims=True) * less
                score_grad = (mixed * (weight_grad - inner)).astype(jnp.bfloat16)
                grad = onto(score_grad, blocks(k_got, b, h))
                qg_ref[at] = ((grad + local_grad[at]) * scale).astype(jnp.bfloat16)
        return 0

    def send_gate(step):
        device = peer_of(step, me, mem_count)
        remote(gate_send, gate_got.at[me], 5, device).start()

    far_first(mem_count, send_gate)
    lax.fori_loop(0, head_count // together, memory_grad, 0)

    arrived = remote(gate_got.at[some], gate_got.at[some], 5, following)
    arrived.wait()
    gate_out_ref[...] = jnp.sum(gate_got[...], axis=0)


def publish(att_ref, qg_ref, gate_ref, att_hbm, qg_hbm, gate_out, sems):
    parts = sems.shape[1]
    size = att_ref.shape[0] // parts
    copies = []
    for i in range(parts):
        rows = pl.ds(i * size, size)
        for which, (ref, hbm) in enumerate(((att_ref, att_hbm), (qg_ref, qg_hbm))):
            copies.append(pltpu.make_async_copy(ref.at[rows], hbm.at[rows], sems.at[which, i]))
    for copy in copies:
        copy.start()
    gate_out[...] = gate_ref[0, : gate_out.shape[0]]
    for copy in copies:
        copy.wait()


def local(
    queries,
    grad_out,
    mem_keys,
    mem_values,
    prev_keys,
    prev_values,
    gate_logit,
    location,
    top_blocks,
    write_slot,
):
    mem_count = lax.axis_size("mem")
    query_count, head_count, pick_count = top_blocks.shape
    stored, block_rows, row_width = mem_keys.shape
    dim = row_width // head_count
    cap = 2
    table_rows = stored + query_count
    any_space = pl.BlockSpec(memory_space=pl.ANY)
    smem = pl.BlockSpec(memory_space=pltpu.SMEM)
    vmem = pl.BlockSpec(memory_space=pltpu.VMEM)
    items = mem_count * cap
    weights_shape = (query_count * head_count, block_rows, pick_count * block_rows)
    attended, query_grad, gate = pl.pallas_call(
        functools.partial(kernel, mem_count, head_count, pick_count),
        out_shape=(
            pltpu.VMEM(queries.shape, jnp.bfloat16),
            pltpu.VMEM(queries.shape, jnp.bfloat16),
            pltpu.VMEM((1, dim), jnp.float32),
        ),
        in_specs=[any_space] * 6 + [smem] * 4,
        out_specs=(vmem, vmem, vmem),
        scratch_shapes=[
            pltpu.VMEM(queries.shape, jnp.bfloat16),
            pltpu.VMEM(queries.shape, jnp.bfloat16),
            pltpu.VMEM((head_count * table_rows, block_rows, dim), jnp.bfloat16),
            pltpu.VMEM((head_count * table_rows, block_rows, dim), jnp.bfloat16),
            pltpu.VMEM((2, block_rows, row_width), jnp.bfloat16),
            pltpu.VMEM((items, block_rows, dim), jnp.bfloat16),
            pltpu.VMEM((items, block_rows, dim), jnp.bfloat16),
            pltpu.VMEM((items, block_rows, dim), jnp.bfloat16),
            pltpu.VMEM((items, block_rows, dim), jnp.bfloat16),
            pltpu.VMEM((mem_count, 1, dim), jnp.int32),
            pltpu.VMEM((mem_count, 1, dim), jnp.int32),
            pltpu.SMEM((mem_count, 1, dim), jnp.int32),
            pltpu.VMEM((2, 1, dim), jnp.int32),
            pltpu.SMEM((2, 1, dim), jnp.int32),
            pltpu.VMEM(queries.shape, jnp.float32),
            pltpu.VMEM(queries.shape, jnp.float32),
            pltpu.VMEM(weights_shape, jnp.bfloat16),
            pltpu.VMEM(weights_shape, jnp.float32),
            pltpu.VMEM((head_count, 1, dim), jnp.float32),
            pltpu.VMEM((1, dim), jnp.float32),
            pltpu.VMEM((mem_count, 1, dim), jnp.float32),
            pltpu.SemaphoreType.DMA((8,)),
            pltpu.SemaphoreType.DMA((6,)),
            pltpu.SemaphoreType.DMA((6,)),
        ],
        compiler_params=pltpu.CompilerParams(
            collective_id=0, has_side_effects=True, vmem_limit_bytes=60 * 2**20
        ),
        name="retrieve_attend",
    )(
        queries,
        grad_out,
        mem_keys,
        mem_values,
        prev_keys,
        prev_values,
        jnp.transpose(top_blocks, (0, 2, 1)),
        location,
        write_slot,
        gate_logit,
    )
    return pl.pallas_call(
        publish,
        out_shape=(
            jax.ShapeDtypeStruct(queries.shape, jnp.bfloat16),
            jax.ShapeDtypeStruct(queries.shape, jnp.bfloat16),
            jax.ShapeDtypeStruct((head_count,), jnp.float32),
        ),
        in_specs=[vmem] * 3,
        out_specs=(any_space, any_space, vmem),
        scratch_shapes=[pltpu.SemaphoreType.DMA((2, 4))],
        name="publish",
    )(*(pltpu.with_memory_space_constraint(x, pltpu.VMEM) for x in (attended, query_grad, gate)))


def solution(mesh):
    in_specs = (
        P(("doc", "mem"), None),
        P(("doc", "mem"), None),
        P(("doc", "mem"), None, None),
        P(("doc", "mem"), None, None),
        P(("doc", "mem"), None, None),
        P(("doc", "mem"), None, None),
        P(),
        P("doc"),
        P(("doc", "mem"), None, None),
        P(("doc", "mem")),
    )
    out_specs = (P(("doc", "mem"), None), P(("doc", "mem"), None), P("doc"))
    return jax.shard_map(local, mesh=mesh, in_specs=in_specs, out_specs=out_specs, check_vma=False)
```

```python
import functools

import jax
import jax.numpy as jnp
from jax import lax
from jax.experimental import pallas as pl
from jax.experimental.pallas import tpu as pltpu
from jax.sharding import PartitionSpec as P

MESH = pl.DeviceIdType.MESH
Z_CHIPS = 8
CORES = 2
LOG2_E = 1.4426950408889634


def route(top_ref, location_ref, write_ref, mem_count, head_count, stored, cap):
    query_count, pick_count, _ = top_ref.shape
    items = query_count * head_count * pick_count
    lane = lax.broadcasted_iota(jnp.int32, (1, items), 1)

    def slots_of(h, slots):
        for b in range(query_count):
            for k in range(pick_count):
                item = (b * head_count + h) * pick_count + k
                slots = jnp.where(lane == item, location_ref[top_ref[b, k, h]], slots)
        return slots

    slots = lax.fori_loop(0, head_count, slots_of, jnp.zeros((1, items), jnp.int32))

    def split(value):
        quotient = lax.shift_right_logical(value * ((1 << 18) // stored + 1), 18)
        return quotient, value - quotient * stored

    owners, inside = split(slots)
    heads = lax.shift_right_logical(lane, pick_count.bit_length() - 1) & (head_count - 1)
    codes = heads * stored + inside
    pairs = slots * head_count + heads
    square = (items, items)
    pair_row = jnp.broadcast_to(pairs, square)
    owner_row = jnp.broadcast_to(owners, square)
    same_pair = pair_row == pair_row.T
    same_owner = owner_row == owner_row.T
    row = lax.broadcasted_iota(jnp.int32, square, 0)
    column = lax.broadcasted_iota(jnp.int32, square, 1)

    def count(condition, axis):
        return jnp.sum(jnp.where(condition, 1, 0), axis=axis, keepdims=True)

    lead_of_row = count(same_pair & (column < row), 1) == 0
    lead_of_column = count(same_pair & (row < column), 0) == 0
    rank_of_row = count(same_owner & (column < row) & lead_of_column, 1)
    position = jnp.sum(
        jnp.where(same_pair & lead_of_row, rank_of_row, 0), axis=0, keepdims=True
    )
    asked_shape = (mem_count, items)
    owner = lax.broadcasted_iota(jnp.int32, asked_shape, 0)
    asked_lane = lax.broadcasted_iota(jnp.int32, asked_shape, 1)
    asked = jnp.zeros(asked_shape, jnp.int32)
    for rank in range(cap):
        match = (owners == owner) & lead_of_column & (position == rank)
        code = jnp.sum(jnp.where(match, codes, 0), axis=1, keepdims=True)
        asked = jnp.where(asked_lane == rank, code, asked)
    head, slot = split(lane)
    place = slot
    for i in range(query_count):
        place = jnp.where(slot == write_ref[i], stored + i, place)
    return asked, owners * cap + position, head * (stored + query_count) + place


def peer_of(step, me, mem_count):
    y_chips = mem_count // (Z_CHIPS * CORES)
    y, z, c = me // (Z_CHIPS * CORES), lax.rem(me // CORES, Z_CHIPS), lax.rem(me, CORES)
    turn = step // Z_CHIPS
    place = lax.rem(step + Z_CHIPS - 1, Z_CHIPS)
    dz = Z_CHIPS // 2 + ((place + 1) // 2) * (1 - 2 * lax.rem(place, 2))
    dy = lax.rem(turn // CORES + 2 * y_chips - dz, y_chips)
    dc = lax.rem(turn, CORES)
    return (lax.rem(y + dy, y_chips) * Z_CHIPS + lax.rem(z + dz, Z_CHIPS)) * CORES + lax.rem(
        c + dc, CORES
    )


def far_first(mem_count, visit):
    turns = mem_count // Z_CHIPS

    def group(places, first_turn):
        def body(turn, _):
            for place in places:
                visit(turn * Z_CHIPS + place + 1)
            return 0

        lax.fori_loop(first_turn, turns, body, 0)

    group((0, 1, 2), 0)
    group((3, 4), 0)
    group((5, 6), 0)
    group((-1,), 1)


def across(a, b):
    return lax.dot_general(a, b, (((1,), (1,)), ((), ())), preferred_element_type=jnp.float32)


def onto(a, b):
    return lax.dot_general(a, b, (((1,), (0,)), ((), ())), preferred_element_type=jnp.float32)


def softmax(raw, scale):
    highest = jnp.max(raw, axis=-1, keepdims=True)
    expanded = jnp.exp2((raw - highest) * (scale * LOG2_E))
    return expanded * (1.0 / jnp.sum(expanded, axis=-1, keepdims=True))


def kernel(
    mem_count,
    head_count,
    pick_count,
    q_hbm,
    g_hbm,
    mk_hbm,
    mv_hbm,
    pk_hbm,
    pv_hbm,
    top_ref,
    location_ref,
    write_ref,
    gate_ref,
    att_ref,
    qg_ref,
    gate_out_ref,
    q_buf,
    g_buf,
    k_table,
    v_table,
    halo,
    k_send,
    v_send,
    k_got,
    v_got,
    codes_ref,
    code_got,
    code_smem,
    spots,
    spots_smem,
    local_out,
    local_grad,
    weights_buf,
    mixed_buf,
    gate_part,
    gate_send,
    gate_got,
    load_sems,
    send_sems,
    recv_sems,
):
    me = lax.axis_index("mem")
    stored, rows, width = mk_hbm.shape
    query_count = pk_hbm.shape[0]
    dim = width // head_count
    scale = dim**-0.5
    cap = 2
    peers = mem_count - 1
    together = 4
    result_heads = 8

    barrier = pltpu.get_barrier_semaphore()

    def greet(step):
        pl.semaphore_signal(
            barrier, inc=1, device_id={"mem": peer_of(step, me, mem_count)}, device_id_type=MESH
        )

    far_first(mem_count, greet)

    table_rows = stored + query_count

    def load_table(source, table, offset, which):
        count = source.shape[0]

        def body(h, _):
            pltpu.make_async_copy(
                source.at[:, :, pl.ds(pl.multiple_of(h * dim, dim), dim)],
                table.at[pl.ds(h * table_rows + offset, count)],
                load_sems.at[which],
            ).start()
            return 0

        lax.fori_loop(0, head_count, body, 0)

    def await_table(source, table, which):
        whole = table.at[pl.ds(0, head_count * source.shape[0])]
        pltpu.make_async_copy(whole, whole, load_sems.at[which]).wait()

    asked, where, place = route(
        top_ref, location_ref, write_ref, mem_count, head_count, stored, cap
    )
    for device in range(mem_count):
        codes_ref[device] = asked[device : device + 1, :]
    spots[0] = where
    spots[1] = place
    code_got[me] = codes_ref[me]

    pl.semaphore_wait(barrier, peers)

    def remote(src, dst, which, device):
        return pltpu.make_async_remote_copy(
            src_ref=src,
            dst_ref=dst,
            send_sem=send_sems.at[which],
            recv_sem=recv_sems.at[which],
            device_id={"mem": device},
            device_id_type=MESH,
        )

    def send_codes(step):
        device = peer_of(step, me, mem_count)
        remote(codes_ref.at[device], code_got.at[me], 0, device).start()

    far_first(mem_count, send_codes)
    spots_copy = pltpu.make_async_copy(spots, spots_smem, load_sems.at[7])
    spots_copy.start()

    following = lax.rem(me + 1, mem_count)
    halo_k = remote(pk_hbm.at[query_count - 1], halo.at[0], 1, following)
    halo_v = remote(pv_hbm.at[query_count - 1], halo.at[1], 2, following)
    halo_k.start()
    halo_v.start()
    load_table(mk_hbm, k_table, 0, 0)
    load_table(pk_hbm, k_table, stored, 1)
    load_table(mv_hbm, v_table, 0, 2)
    load_table(pv_hbm, v_table, stored, 3)
    loads = [
        pltpu.make_async_copy(q_hbm, q_buf, load_sems.at[4]),
        pltpu.make_async_copy(g_hbm, g_buf, load_sems.at[5]),
    ]
    for load in loads:
        load.start()

    some = pl.ds(0, peers)
    remote(codes_ref.at[some], code_got.at[some], 0, following).wait()
    code_copy = pltpu.make_async_copy(code_got, code_smem, load_sems.at[6])
    code_copy.start()
    await_table(mk_hbm, k_table, 0)
    await_table(pk_hbm, k_table, 1)
    code_copy.wait()
    spots_copy.wait()

    def gather(table, device, out, at):
        for rank in range(cap):
            out[at + rank] = table[spots_smem[1, 0, code_smem[device, 0, rank]]]

    def serve(table, out, got, which):
        gather(table, peer_of(1, me, mem_count), out, cap)

        def send(step):
            device = peer_of(step, me, mem_count)
            remote(
                out.at[pl.ds(step * cap, cap)], got.at[pl.ds(me * cap, cap)], which, device
            ).start()

        def body(step, _):
            gather(table, peer_of(step, me, mem_count), out, step * cap)
            send(step - 1)
            return 0

        lax.fori_loop(2, mem_count, body, 0)
        gather(table, me, got, me * cap)
        send(peers)

    serve(k_table, k_send, k_got, 3)
    await_table(mv_hbm, v_table, 2)
    await_table(pv_hbm, v_table, 3)
    serve(v_table, v_send, v_got, 4)

    for load in loads:
        load.wait()
    halo_k.wait()
    halo_v.wait()

    first = me == 0

    def places(b, h):
        return pl.ds(b * rows, rows), pl.ds(pl.multiple_of(h * dim, dim), dim)

    def mix_of(h):
        return 1.0 / (1.0 + jnp.exp(-jnp.full((1, dim), gate_ref[h], jnp.float32)))

    def local_head(h, _):
        columns = pl.ds(pl.multiple_of(h * dim, dim), dim)
        own = h * table_rows + stored
        rest = 1.0 - mix_of(h)
        part = jnp.zeros((1, dim), jnp.float32)
        for b in range(query_count):
            at = places(b, h)
            q, g = q_buf[at], g_buf[at]
            if b == 0:
                older_k, older_v = halo[0, :, columns], halo[1, :, columns]
            else:
                older_k, older_v = k_table[own + b - 1], v_table[own + b - 1]
            keys = jnp.concatenate([older_k, k_table[own + b]], axis=0)
            values = jnp.concatenate([older_v, v_table[own + b]], axis=0)
            raw = across(q, keys)
            if b == 0:
                column_ids = lax.broadcasted_iota(jnp.int32, raw.shape, 1)
                raw = jnp.where(first & (column_ids < rows), -jnp.inf, raw)
            weights = softmax(raw, scale)
            result = onto(weights.astype(jnp.bfloat16), values)
            weight_grad = across(g, values)
            inner = jnp.sum(weights * weight_grad, axis=-1, keepdims=True)
            score_grad = weights * (weight_grad - inner) * rest[:, :1]
            local_grad[at] = onto(score_grad.astype(jnp.bfloat16), keys)
            local_out[at] = result * rest
            part = part - jnp.sum(g.astype(jnp.float32) * result, axis=0, keepdims=True)
        gate_part[h] = part
        return 0

    lax.fori_loop(0, head_count, local_head, 0)

    def blocks(got, b, h):
        first_item = (b * head_count + h) * pick_count
        return jnp.concatenate([got[spots_smem[0, 0, first_item + k]] for k in range(pick_count)], axis=0)

    everyone = pl.ds(0, peers * cap)
    remote(k_send.at[everyone], k_got.at[everyone], 3, following).wait()

    def memory_weights(h, _):
        mix = mix_of(h)[:, :1]
        for b in range(query_count):
            raw = across(q_buf[places(b, h)], blocks(k_got, b, h))
            weights = softmax(raw, scale)
            weights_buf[b * head_count + h] = weights.astype(jnp.bfloat16)
            mixed_buf[b * head_count + h] = weights * mix
        return 0

    lax.fori_loop(0, head_count, memory_weights, 0)

    remote(v_send.at[everyone], v_got.at[everyone], 4, following).wait()

    def memory_result(step, _):
        for h in [step * result_heads + i for i in range(result_heads)]:
            mix = mix_of(h)
            part = gate_part[h]
            for b in range(query_count):
                at = places(b, h)
                result = onto(weights_buf[b * head_count + h], blocks(v_got, b, h))
                att_ref[at] = (mix * result + local_out[at]).astype(jnp.bfloat16)
                part = part + jnp.sum(
                    g_buf[at].astype(jnp.float32) * result, axis=0, keepdims=True
                )
            gate_part[h] = part
        return 0

    lax.fori_loop(0, head_count // result_heads, memory_result, 0)

    lane_ids = lax.broadcasted_iota(jnp.int32, (1, dim), 1)
    total = jnp.zeros((1, dim), jnp.float32)
    for h in range(head_count):
        mix = mix_of(h)
        term = jnp.sum(gate_part[h], axis=-1, keepdims=True) * (mix * (1.0 - mix))
        total = jnp.where(lane_ids == h, term, total)
    gate_send[...] = total
    gate_got[me] = total

    def memory_grad(step, _):
        for h in [step * together + i for i in range(together)]:
            less = 1.0 + jnp.exp(-jnp.full((1, 1), gate_ref[h], jnp.float32))
            for b in range(query_count):
                at = places(b, h)
                mixed = mixed_buf[b * head_count + h]
                weight_grad = across(g_buf[at], blocks(v_got, b, h))
                inner = jnp.sum(mixed * weight_grad, axis=-1, keepdims=True) * less
                score_grad = (mixed * (weight_grad - inner)).astype(jnp.bfloat16)
                grad = onto(score_grad, blocks(k_got, b, h))
                qg_ref[at] = ((grad + local_grad[at]) * scale).astype(jnp.bfloat16)
        return 0

    def send_gate(step):
        device = peer_of(step, me, mem_count)
        remote(gate_send, gate_got.at[me], 5, device).start()

    far_first(mem_count, send_gate)
    lax.fori_loop(0, head_count // together, memory_grad, 0)

    arrived = remote(gate_got.at[some], gate_got.at[some], 5, following)
    arrived.wait()
    gate_out_ref[...] = jnp.sum(gate_got[...], axis=0)


def publish(att_ref, qg_ref, gate_ref, att_hbm, qg_hbm, gate_out, sems):
    parts = sems.shape[1]
    size = att_ref.shape[0] // parts
    copies = []
    for i in range(parts):
        rows = pl.ds(i * size, size)
        for which, (ref, hbm) in enumerate(((att_ref, att_hbm), (qg_ref, qg_hbm))):
            copies.append(pltpu.make_async_copy(ref.at[rows], hbm.at[rows], sems.at[which, i]))
    for copy in copies:
        copy.start()
    gate_out[...] = gate_ref[0, : gate_out.shape[0]]
    for copy in copies:
        copy.wait()


def local(
    queries,
    grad_out,
    mem_keys,
    mem_values,
    prev_keys,
    prev_values,
    gate_logit,
    location,
    top_blocks,
    write_slot,
):
    mem_count = lax.axis_size("mem")
    query_count, head_count, pick_count = top_blocks.shape
    stored, block_rows, row_width = mem_keys.shape
    dim = row_width // head_count
    cap = 2
    table_rows = stored + query_count
    any_space = pl.BlockSpec(memory_space=pl.ANY)
    smem = pl.BlockSpec(memory_space=pltpu.SMEM)
    vmem = pl.BlockSpec(memory_space=pltpu.VMEM)
    items = mem_count * cap
    weights_shape = (query_count * head_count, block_rows, pick_count * block_rows)
    attended, query_grad, gate = pl.pallas_call(
        functools.partial(kernel, mem_count, head_count, pick_count),
        out_shape=(
            pltpu.VMEM(queries.shape, jnp.bfloat16),
            pltpu.VMEM(queries.shape, jnp.bfloat16),
            pltpu.VMEM((1, dim), jnp.float32),
        ),
        in_specs=[any_space] * 6 + [smem] * 4,
        out_specs=(vmem, vmem, vmem),
        scratch_shapes=[
            pltpu.VMEM(queries.shape, jnp.bfloat16),
            pltpu.VMEM(queries.shape, jnp.bfloat16),
            pltpu.VMEM((head_count * table_rows, block_rows, dim), jnp.bfloat16),
            pltpu.VMEM((head_count * table_rows, block_rows, dim), jnp.bfloat16),
            pltpu.VMEM((2, block_rows, row_width), jnp.bfloat16),
            pltpu.VMEM((items, block_rows, dim), jnp.bfloat16),
            pltpu.VMEM((items, block_rows, dim), jnp.bfloat16),
            pltpu.VMEM((items, block_rows, dim), jnp.bfloat16),
            pltpu.VMEM((items, block_rows, dim), jnp.bfloat16),
            pltpu.VMEM((mem_count, 1, dim), jnp.int32),
            pltpu.VMEM((mem_count, 1, dim), jnp.int32),
            pltpu.SMEM((mem_count, 1, dim), jnp.int32),
            pltpu.VMEM((2, 1, dim), jnp.int32),
            pltpu.SMEM((2, 1, dim), jnp.int32),
            pltpu.VMEM(queries.shape, jnp.float32),
            pltpu.VMEM(queries.shape, jnp.float32),
            pltpu.VMEM(weights_shape, jnp.bfloat16),
            pltpu.VMEM(weights_shape, jnp.float32),
            pltpu.VMEM((head_count, 1, dim), jnp.float32),
            pltpu.VMEM((1, dim), jnp.float32),
            pltpu.VMEM((mem_count, 1, dim), jnp.float32),
            pltpu.SemaphoreType.DMA((8,)),
            pltpu.SemaphoreType.DMA((6,)),
            pltpu.SemaphoreType.DMA((6,)),
        ],
        compiler_params=pltpu.CompilerParams(
            collective_id=0, has_side_effects=True, vmem_limit_bytes=60 * 2**20
        ),
        name="retrieve_attend",
    )(
        queries,
        grad_out,
        mem_keys,
        mem_values,
        prev_keys,
        prev_values,
        jnp.transpose(top_blocks, (0, 2, 1)),
        location,
        write_slot,
        gate_logit,
    )
    return pl.pallas_call(
        publish,
        out_shape=(
            jax.ShapeDtypeStruct(queries.shape, jnp.bfloat16),
            jax.ShapeDtypeStruct(queries.shape, jnp.bfloat16),
            jax.ShapeDtypeStruct((head_count,), jnp.float32),
        ),
        in_specs=[vmem] * 3,
        out_specs=(any_space, any_space, vmem),
        scratch_shapes=[pltpu.SemaphoreType.DMA((2, 4))],
        name="publish",
    )(*(pltpu.with_memory_space_constraint(x, pltpu.VMEM) for x in (attended, query_grad, gate)))


def solution(mesh):
    in_specs = (
        P(("doc", "mem"), None),
        P(("doc", "mem"), None),
        P(("doc", "mem"), None, None),
        P(("doc", "mem"), None, None),
        P(("doc", "mem"), None, None),
        P(("doc", "mem"), None, None),
        P(),
        P("doc"),
        P(("doc", "mem"), None, None),
        P(("doc", "mem")),
    )
    out_specs = (P(("doc", "mem"), None), P(("doc", "mem"), None), P("doc"))
    return jax.shard_map(local, mesh=mesh, in_specs=in_specs, out_specs=out_specs, check_vma=False)
```
